32 devices in a mesh: gx: 8 (over z, x), gy: 4 (over y, core).
Axes of the slice: x: 2, y: 2, z: 4, core: 2. Of those that a mesh axis runs over, the one named last changes fastest.
Arguments:
- start_field: bfloat16 [6, 1280, 1024], P(None, 'gx', 'gy'), may hold values from -6 to 6
- tensor: bfloat16 [6, 1280, 1024], P(None, 'gx', 'gy'), may hold values from -6 to 20, as said below
- class_map: int32 [80, 64], P('gx', 'gy'), may hold values from 0 to 1, as said below
Outputs:
- mode_field: float32 [6, 1280, 1024], P(None, 'gx', 'gy')
- estimate: float32 [], replicated
The draws below stay inside these ranges and needn't reach their ends.
Inputs may be any that keep to these rules, and one draw needn't show every extreme that they name: `tensor`: entries 0 to 2 of a cell are positive, entries 3 to 5 are its off-diagonal entries. `class_map`: 1 marks a tile whose cells use the full tensor, 0 a tile that uses its diagonal only.
All inputs are finite; a program needn't handle non-finite values.
Results may differ from the reference program's by a relative error of at most 0.00035.
Values may be sent and summed in bfloat16 or wider, within the bound.
No kernel may reach another device: no remote copies, remote signals or barrier semaphores. Data moves between devices by JAX's collectives and lax.ppermute only.
A program may use at most 64 MiB of HBM per device.

```python
import math
import jax
import jax.numpy as jnp
from jax import lax

CX = 160
CY = 256
TILE = 16
ITERS = 4
NX = 1280
NY = 1024


def draw_tensor(key, part):
    subkeys = jax.random.split(jax.random.fold_in(key, 11), 3)
    row_pos = jnp.arange(NX, dtype=jnp.float32)[:, None] / NX
    col_pos = jnp.arange(NY, dtype=jnp.float32)[None, :] / NY
    rising = jnp.exp(math.log(1.15) * row_pos + math.log(1.5) * col_pos)
    base_scale = jnp.exp(jax.random.uniform(subkeys[0], (NX, NY), jnp.float32, math.log(0.4), math.log(2.5)))
    channel_gain = jnp.exp(jax.random.uniform(subkeys[1], (3, NX, NY), jnp.float32, math.log(0.75), math.log(1.333)))
    diagonal = base_scale[None] * rising[None] * channel_gain
    off_spread = jax.random.uniform(subkeys[2], (3, NX, NY), jnp.float32, -1.0, 1.0)
    off_xy = 0.3 * off_spread[0] * jnp.sqrt(diagonal[0] * diagonal[1])
    off_xz = 0.3 * off_spread[1] * jnp.sqrt(diagonal[0] * diagonal[2])
    off_yz = 0.3 * off_spread[2] * jnp.sqrt(diagonal[1] * diagonal[2])
    whole = jnp.concatenate([diagonal, jnp.stack([off_xy, off_xz, off_yz])], axis=0)
    return whole.astype(jnp.bfloat16)


def draw_class_map(key, part):
    subkeys = jax.random.split(jax.random.fold_in(key, 23), 2)
    blocks_x = NX // CX
    blocks_y = NY // CY
    threshold = jax.random.randint(subkeys[0], (blocks_x, 1, blocks_y, 1), 100, 700)
    tickets = jax.random.randint(subkeys[1], (blocks_x, CX // TILE, blocks_y, CY // TILE), 0, 1000)
    marked = (tickets < threshold).astype(jnp.int32)
    return marked.reshape(NX // TILE, NY // TILE)


def block_levels(own_key, extent, cuts, least, top_value):
    gain, own = 1.0, jax.random.fold_in(own_key, 6)
    for position, blocks in cuts:
        steps = jnp.exp(jax.random.uniform(jax.random.fold_in(own, position), (blocks,), jnp.float32, least / len(cuts), top_value / len(cuts)))
        gain = gain * jnp.repeat(steps, extent[position] // blocks).reshape([-1 if axis == position else 1 for axis in range(len(extent))])
    return gain


def gaussian(stream_key, extent, scale, limit, shards=(), kind=jnp.bfloat16):
    level = block_levels(stream_key, extent, shards, -0.22, 0.18) if shards else 1.0
    result = jax.random.normal(stream_key, extent, jnp.float32) * scale * level
    return jnp.minimum(jnp.maximum(result, -limit), limit).astype(kind)


def setup_inputs(seed: int = 0) -> dict:
    seeds = jax.random.split(jax.random.key(seed), 4)
    return {
        "start_field": gaussian(seeds[0], (6, NX, NY), 1.0, 6.0, ((1, 8), (2, 4))),
        "tensor": draw_tensor(jax.random.fold_in(seeds[3], 71), 0),
        "class_map": draw_class_map(jax.random.fold_in(seeds[3], 71), 0),
    }


epsilon = 1e-06
wave_number = 0.75
near_weight = 1.125
far_weight = 1.0 / 24.0

def differ(array, dimension):
    length = array.shape[dimension]

    def offset_slice(offset):
        return lax.slice_in_dim(array, offset, length - 3 + offset, axis=dimension)
    return near_weight * (offset_slice(2) - offset_slice(1)) - far_weight * (offset_slice(3) - offset_slice(0))

def trimmed(array, dimension, lower_cut, upper_cut):
    return lax.slice_in_dim(array, lower_cut, array.shape[dimension] - upper_cut, axis=dimension)

def rotate(values):
    return wave_number * jnp.stack([-values[1], values[0]])

def curl_step(current, lower_cut, upper_cut):
    halves = current.reshape(2, 3, current.shape[1], current.shape[2])
    comp_x, comp_y, comp_z = (halves[:, 0], halves[:, 1], halves[:, 2])

    def along_x(values):
        return trimmed(differ(values, 1), 2, lower_cut, upper_cut)

    def along_y(values):
        return trimmed(differ(values, 2), 1, lower_cut, upper_cut)

    def centre(values):
        return trimmed(trimmed(values, 1, lower_cut, upper_cut), 2, lower_cut, upper_cut)
    out_x = along_y(comp_z) - rotate(centre(comp_y))
    out_y = rotate(centre(comp_x)) - along_x(comp_z)
    out_z = along_x(comp_y) - along_y(comp_x)
    stacked = jnp.stack([out_x, out_y, out_z], axis=1)
    return stacked.reshape(6, stacked.shape[2], stacked.shape[3])

def heavy_cells(class_map):
    tiles_x, tiles_y = class_map.shape
    spread = jnp.broadcast_to(class_map.astype(jnp.float32)[:, None, :, None], (tiles_x, TILE, tiles_y, TILE))
    return spread.reshape(tiles_x * TILE, tiles_y * TILE)

def apply_tensor(curled, tensor, heavy_mask):
    halves = curled.reshape(2, 3, curled.shape[1], curled.shape[2])
    entries = tensor.astype(jnp.float32)
    cur_x, cur_y, cur_z = (halves[:, 0], halves[:, 1], halves[:, 2])
    out_x = entries[0] * cur_x + heavy_mask * (entries[3] * cur_y + entries[4] * cur_z)
    out_y = entries[1] * cur_y + heavy_mask * (entries[3] * cur_x + entries[5] * cur_z)
    out_z = entries[2] * cur_z + heavy_mask * (entries[4] * cur_x + entries[5] * cur_y)
    stacked = jnp.stack([out_x, out_y, out_z], axis=1)
    return stacked.reshape(6, curled.shape[1], curled.shape[2])

def operate(current, tensor, heavy_mask):
    padded = jnp.pad(current, ((0, 0), (1, 2), (1, 2)))
    magnetic = curl_step(padded, 1, 2)
    padded = jnp.pad(magnetic, ((0, 0), (2, 1), (2, 1)))
    return apply_tensor(curl_step(padded, 2, 1), tensor, heavy_mask)

def reference(start_field, tensor, class_map):
    heavy_mask = heavy_cells(class_map)
    cell_count = NX * NY
    current = start_field.astype(jnp.float32)
    for turn_index in range(ITERS):
        image_field = operate(current, tensor, heavy_mask)
        square_sum = jnp.sum(image_field * image_field)
        current = image_field * lax.rsqrt(square_sum / cell_count + epsilon)
    image_field = operate(current, tensor, heavy_mask)
    estimate = jnp.sum(current * image_field) / jnp.sum(current * current)
    return (current, estimate)
```

```python
import jax
import jax.numpy as jnp
from jax import lax
from jax.experimental import pallas as pl
from jax.experimental.pallas import tpu as pltpu
from jax.sharding import PartitionSpec as P

TILE = 16
ITERS = 4
LANES = 128
SUB = 8
STRIP = 16
LOW = 13
HIGH = 14
PAD = 24
epsilon = 1e-06
f32 = jnp.float32
bf16 = jnp.bfloat16
FIELD_SCALE = (18.0, 18.0, 1.0, 18.0, 18.0, 1.0)
TENSOR_SCALE = (
    1.0 / 576.0,
    1.0 / 576.0,
    1.0 / (576.0 * 324.0),
    1.0 / 576.0,
    1.0 / (576.0 * 18.0),
    1.0 / (576.0 * 18.0),
)
BELOW = 324.0


def lane_index(rows):
    return lax.broadcasted_iota(jnp.int32, (rows, LANES), 1)


def shifted(value, amount):
    amount = amount % LANES
    return value if amount == 0 else pltpu.roll(value, amount, 1)


def heavy_cells(class_map, rows, cols):
    tiles_x, tiles_y = class_map.shape
    row_of = lax.broadcasted_iota(jnp.int32, (rows, tiles_x), 0) // TILE
    row_pick = (row_of == lax.broadcasted_iota(jnp.int32, (rows, tiles_x), 1)).astype(f32)
    col_of = lax.broadcasted_iota(jnp.int32, (tiles_y, cols), 1) // TILE
    col_pick = (col_of == lax.broadcasted_iota(jnp.int32, (tiles_y, cols), 0)).astype(f32)
    spread = jnp.dot(row_pick, class_map.astype(f32), preferred_element_type=f32)
    return jnp.dot(spread, col_pick, preferred_element_type=f32)


def pack_kernel(start, tensor, class_map, left, right, top, bottom, mask):
    rows, cols = start.shape[1:]
    mask[...] = heavy_cells(class_map[...], rows, cols)

    def source(index, first):
        if index < 6:
            return start[index, pl.ds(first, STRIP), :].astype(f32)
        value = tensor[index - 6, pl.ds(first, STRIP), :].astype(f32)
        if index >= 9:
            value = value * mask[pl.ds(first, STRIP), :]
        return value

    lanes = lane_index(STRIP)
    last = cols - LANES
    per = LANES // STRIP

    def block(step, carry):
        first = pl.multiple_of(step * STRIP, STRIP)
        for group in range(2):
            low_part = jnp.zeros((STRIP, LANES), f32)
            high_part = jnp.zeros((STRIP, LANES), f32)
            for index in range(group * per, min(12, (group + 1) * per)):
                value = source(index, first)
                place = STRIP * (index % per)
                here = (lanes >= place) & (lanes < place + STRIP)
                low_part = jnp.where(here, shifted(value[:, :LANES], place), low_part)
                high_part = jnp.where(here, shifted(value[:, last:], place + STRIP), high_part)
            left[pl.ds(first, STRIP), group * LANES : (group + 1) * LANES] = low_part.astype(bf16)
            right[pl.ds(first, STRIP), group * LANES : (group + 1) * LANES] = high_part.astype(bf16)
        return carry

    lax.fori_loop(0, rows // STRIP, block, 0)
    for index in range(12):
        top[index * STRIP : (index + 1) * STRIP, :] = source(index, 0).astype(bf16)
        bottom[index * STRIP : (index + 1) * STRIP, :] = source(index, rows - STRIP).astype(bf16)


def forward(centre, plus, plus2, minus):
    return 27.0 * (plus - centre) - (plus2 - minus)


def main_kernel(
    row_parts, width, start, tensor, class_map, left, right, above, below, out, sums, field, flux, coef, mask, keep, keep2, inner
):
    rows, cols = start.shape[1:]
    tiles = field.shape[0]
    per = LANES // STRIP
    row_base = lax.axis_index("gx") * rows
    col_base = lax.axis_index("gy") * cols
    total_rows = rows * lax.axis_size("gx")
    total_cols = cols * lax.axis_size("gy")
    mask[...] = heavy_cells(class_map[...], rows, cols)
    deep = field.shape[2]

    for tile in range(tiles):
        r = lax.broadcasted_iota(jnp.int32, (deep, LANES), 0) - PAD
        c = lax.broadcasted_iota(jnp.int32, (deep, LANES), 1) + (tile * width - LOW)
        gr, gc = r + row_base, c + col_base
        good = (gr >= 0) & (gr < total_rows) & (gc >= 0) & (gc < total_cols)
        keep[tile] = jnp.where(good, 1.0, 0.0)
        keep2[tile] = jnp.where(good, BELOW, 0.0)
        lo = tile * width
        mine = (r >= 0) & (r < rows) & (c >= lo) & (c < min(cols, lo + width))
        inner[tile] = jnp.where(mine, 1.0, 0.0)
        edge = jnp.zeros((SUB, LANES), f32)
        for index in range(6):
            for first in (0, deep - SUB):
                field[tile, index, first : first + SUB, :] = edge
                flux[tile, index, first : first + SUB, :] = edge

    lanes = lane_index(STRIP)

    def place(target, index, first, value, low_strip, high_strip, factor):
        value = value * factor
        spot = STRIP * (index % per)
        group = index // per
        low_part = low_strip[:, group * LANES : (group + 1) * LANES] * factor
        high_part = high_strip[:, group * LANES : (group + 1) * LANES] * factor
        which = index if index < 6 else index - 6
        for tile in range(tiles):
            base = tile * width - LOW
            result = jnp.zeros((STRIP, LANES), f32)
            if base < 0:
                result = jnp.where(lanes < -base, shifted(low_part, -(spot + STRIP + base)), result)
            for piece in range(cols // LANES):
                begin = piece * LANES - base
                if begin >= LANES or begin + LANES <= 0:
                    continue
                here = (lanes >= begin) & (lanes < begin + LANES)
                moved = shifted(value[:, piece * LANES : (piece + 1) * LANES], begin)
                result = jnp.where(here, moved, result)
            begin = cols - base
            if begin < LANES:
                here = (lanes >= begin) & (lanes < begin + STRIP)
                result = jnp.where(here, shifted(high_part, begin - spot), result)
            target[tile, which, pl.ds(first, STRIP), :] = result

    def assemble(step, carry):
        first = pl.multiple_of(step * STRIP, STRIP)
        low_strip = left[pl.ds(first, STRIP), :].astype(f32)
        high_strip = right[pl.ds(first, STRIP), :].astype(f32)
        for index in range(12):
            if index < 6:
                value = start[index, pl.ds(first, STRIP), :].astype(f32)
                place(field, index, PAD + first, value, low_strip, high_strip, FIELD_SCALE[index])
            else:
                value = tensor[index - 6, pl.ds(first, STRIP), :].astype(f32)
                if index >= 9:
                    value = value * mask[pl.ds(first, STRIP), :]
                place(coef, index, PAD + first, value, low_strip, high_strip, TENSOR_SCALE[index - 6])
        return carry

    lax.fori_loop(0, rows // STRIP, assemble, 0)
    for strip, first in ((above, PAD - STRIP), (below, PAD + rows)):
        low_strip = strip[12 * STRIP : 13 * STRIP, :].astype(f32)
        high_strip = strip[13 * STRIP : 14 * STRIP, :].astype(f32)
        for index in range(12):
            value = strip[index * STRIP : (index + 1) * STRIP, :].astype(f32)
            factor = FIELD_SCALE[index] if index < 6 else TENSOR_SCALE[index - 6]
            place(field if index < 6 else coef, index, first, value, low_strip, high_strip, factor)

    def load(ref, tile, index, first, offset):
        return ref[tile, index, pl.ds(first + offset, SUB), :]

    def curl_forward(ref, tile, first):
        out_parts = []
        centre = [load(ref, tile, index, first, 0) for index in range(6)]
        for part in range(2):
            sign = 1.0 if part == 0 else -1.0
            x, y, z = centre[3 * part : 3 * part + 3]
            ox, oy = centre[3 - 3 * part], centre[4 - 3 * part]
            zi, yi = 3 * part + 2, 3 * part + 1
            dyz = forward(z, shifted(z, -1), shifted(z, -2), shifted(z, 1))
            dxz = forward(
                z, load(ref, tile, zi, first, 1), load(ref, tile, zi, first, 2), load(ref, tile, zi, first, -1)
            )
            near = (load(ref, tile, yi, first, 1) - y) - (shifted(x, -1) - x)
            far = (load(ref, tile, yi, first, 2) - load(ref, tile, yi, first, -1)) - (shifted(x, -2) - shifted(x, 1))
            if part == 0:
                out_parts.append((dyz + oy, -(ox + dxz), 27.0 * near - far))
            else:
                out_parts.append((dyz - oy, ox - dxz, 27.0 * near - far))
        return out_parts

    def curl_backward(ref, tile, first):
        out_parts = []
        centre = [load(ref, tile, index, first, 0) for index in range(6)]
        for part in range(2):
            x, y, z = centre[3 * part : 3 * part + 3]
            ox, oy = centre[3 - 3 * part], centre[4 - 3 * part]
            zi, yi = 3 * part + 2, 3 * part + 1
            dyz = forward(shifted(z, 1), z, shifted(z, -1), shifted(z, 2))
            dxz = forward(
                load(ref, tile, zi, first, -1), z, load(ref, tile, zi, first, 1), load(ref, tile, zi, first, -2)
            )
            near = (y - load(ref, tile, yi, first, -1)) - (x - shifted(x, 1))
            far = (load(ref, tile, yi, first, 1) - load(ref, tile, yi, first, -2)) - (shifted(x, -1) - shifted(x, 2))
            if part == 0:
                out_parts.append((dyz + oy, -(ox + dxz), 27.0 * near - far))
            else:
                out_parts.append((dyz - oy, ox - dxz, 27.0 * near - far))
        return out_parts

    def contract(tile, first, parts):
        k = [load(coef, tile, index, first, 0) for index in range(6)]
        results = []
        for cx, cy, cz in parts:
            results.append(
                (
                    k[0] * cx + k[3] * cy + k[4] * cz,
                    k[3] * cx + k[1] * cy + k[5] * cz,
                    k[4] * cx + k[5] * cy + k[2] * cz,
                )
            )
        return results

    unroll = 4

    def over(span, body, carry):
        lo = (PAD + span[0]) // SUB * SUB
        hi = -(-(PAD + span[1]) // SUB) * SUB
        count = (hi - lo) // SUB

        def chunk(size, at, carry):
            for inside in range(size):
                carry = body(at + inside * SUB, carry)
            return carry

        whole = count // unroll

        def loop(step, carry):
            return chunk(unroll, pl.multiple_of(lo + step * (unroll * SUB), SUB), carry)

        carry = lax.fori_loop(0, whole, loop, carry)
        if count % unroll:
            carry = chunk(count % unroll, lo + whole * unroll * SUB, carry)
        return carry

    zero = jnp.zeros((SUB, LANES), f32)

    def run_tile(tile, totals):
        totals = list(totals)
        for turn in range(ITERS):
            reach = 3 * (ITERS - 1 - turn)

            def first_half(first, carry):
                m, m2 = keep[tile, pl.ds(first, SUB), :], keep2[tile, pl.ds(first, SUB), :]
                for part, (hx, hy, hz) in enumerate(curl_forward(field, tile, first)):
                    flux[tile, 3 * part, pl.ds(first, SUB), :] = hx * m2
                    flux[tile, 3 * part + 1, pl.ds(first, SUB), :] = hy * m2
                    flux[tile, 3 * part + 2, pl.ds(first, SUB), :] = hz * m
                return carry

            over((-3 - reach, rows + 3 + reach), first_half, 0)

            def second_half(first, carry):
                flat, upright = carry
                results = contract(tile, first, curl_backward(flux, tile, first))
                for part, triple in enumerate(results):
                    for axis in range(3):
                        field[tile, 3 * part + axis, pl.ds(first, SUB), :] = triple[axis]
                (ax, ay, az), (bx, by, bz) = results
                own = inner[tile, pl.ds(first, SUB), :]
                flat = flat + own * ((ax * ax + ay * ay) + (bx * bx + by * by))
                upright = upright + own * (az * az + bz * bz)
                return flat, upright

            flat, upright = over((-1 - reach, rows + 2 + reach), second_half, (zero, zero))
            totals[turn] = totals[turn] + (flat * (1.0 / 324.0) + upright)

        def weigh(first, carry):
            e = [load(field, tile, index, first, 0) for index in range(6)]
            parts = contract(tile, first, ((e[0], e[1], BELOW * e[2]), (e[3], e[4], BELOW * e[5])))
            for part, triple in enumerate(parts):
                for axis in range(3):
                    flux[tile, 3 * part + axis, pl.ds(first, SUB), :] = triple[axis]
            return carry

        over((-1, rows + 2), weigh, 0)

        def pair(first, carry):
            flat, upright = carry
            one = curl_forward(field, tile, first)
            two = curl_forward(flux, tile, first)
            own = inner[tile, pl.ds(first, SUB), :]
            flat = flat + own * (
                (one[0][0] * two[0][0] + one[0][1] * two[0][1]) + (one[1][0] * two[1][0] + one[1][1] * two[1][1])
            )
            upright = upright + own * (one[0][2] * two[0][2] + one[1][2] * two[1][2])
            return flat, upright

        flat, upright = over((0, rows), pair, (zero, zero))
        totals[ITERS] = totals[ITERS] + (flat + upright * (1.0 / 324.0))
        return tuple(totals)

    totals = lax.fori_loop(0, tiles, run_tile, (zero,) * (ITERS + 1))

    line_lanes = lax.broadcasted_iota(jnp.int32, (1, LANES), 1)
    line = jnp.zeros((1, LANES), f32)
    for number, total in enumerate(totals):
        amount = jnp.sum(jnp.sum(total, axis=0, keepdims=True), axis=1, keepdims=True)
        line = jnp.where(line_lanes == number, amount, line)
    sums[...] = jnp.broadcast_to(line, sums.shape)

    sub_lanes = lane_index(SUB)

    def collect(step, carry):
        first = pl.multiple_of(step * SUB, SUB)
        for index in range(6):
            for piece in range(cols // LANES):
                result = zero
                for tile in range(tiles):
                    begin = tile * width - piece * LANES
                    end = min(cols, (tile + 1) * width) - piece * LANES
                    if end <= 0 or begin >= LANES:
                        continue
                    moved = shifted(field[tile, index, pl.ds(PAD + first, SUB), :], begin - LOW)
                    here = (sub_lanes >= begin) & (sub_lanes < end)
                    result = jnp.where(here, moved, result)
                out[index, pl.ds(first, SUB), piece * LANES : (piece + 1) * LANES] = result
        return carry

    lax.fori_loop(0, rows // SUB, collect, 0)


def scale_kernel(cell_count, field, sums, out, estimate):
    totals = jnp.sum(sums[...], axis=0, keepdims=True)
    picks = [totals[:, number : number + 1] for number in range(ITERS + 1)]
    factor = jnp.ones((1, 1), f32)
    for number in range(ITERS):
        square_sum = factor * factor * picks[number]
        factor = factor * lax.rsqrt(square_sum / cell_count + epsilon)
    estimate[...] = picks[ITERS] / picks[ITERS - 1]
    flat = factor * (1.0 / 18.0)
    for index in range(6):
        out[index] = field[index] * (factor if index % 3 == 2 else flat)


def on_device(start_field, tensor, class_map):
    rows, cols = start_field.shape[1:]
    devices = lax.axis_size("gx") * lax.axis_size("gy")
    cell_count = rows * cols * devices
    tiles = -(-cols // (LANES - LOW - HIGH))
    width = -(-cols // tiles)
    whole = pl.BlockSpec(memory_space=pltpu.VMEM)
    strip_rows = 12 * STRIP
    left, right, top, bottom = pl.pallas_call(
        pack_kernel,
        out_shape=(
            jax.ShapeDtypeStruct((rows, 2 * LANES), bf16),
            jax.ShapeDtypeStruct((rows, 2 * LANES), bf16),
            jax.ShapeDtypeStruct((strip_rows, cols), bf16),
            jax.ShapeDtypeStruct((strip_rows, cols), bf16),
        ),
        in_specs=[whole] * 3,
        out_specs=(whole,) * 4,
        scratch_shapes=[pltpu.VMEM((rows, cols), f32)],
        name="pack",
    )(start_field, tensor, class_map)

    def both(low_going, high_going, axis):
        count = lax.axis_size(axis)
        up = [(i, i + 1) for i in range(count - 1)]
        down = [(j, i) for i, j in up]
        return lax.ppermute(high_going, axis, up), lax.ppermute(low_going, axis, down)

    from_left, from_right = both(left, right, "gy")
    top = jnp.concatenate([top, from_left[:STRIP], from_right[:STRIP]])
    bottom = jnp.concatenate([bottom, from_left[-STRIP:], from_right[-STRIP:]])
    above, below = both(top, bottom, "gx")
    deep = rows + 2 * PAD
    plane = pltpu.VMEM((tiles, deep, LANES), f32)
    stack = pltpu.VMEM((tiles, 6, deep, LANES), f32)

    def main(*refs):
        main_kernel(None, width, *refs)

    image, sums = pl.pallas_call(
        main,
        out_shape=(
            jax.ShapeDtypeStruct((6, rows, cols), f32),
            jax.ShapeDtypeStruct((devices, LANES), f32),
        ),
        in_specs=[whole] * 7,
        out_specs=(whole,) * 2,
        scratch_shapes=[stack, stack, stack, pltpu.VMEM((rows, cols), f32), plane, plane, plane],
        name="products",
    )(start_field, tensor, class_map, from_left, from_right, above, below)
    sums = lax.all_to_all(sums, ("gx", "gy"), 0, 0, tiled=True)

    def scale(*refs):
        scale_kernel(float(cell_count), *refs)

    mode, estimate = pl.pallas_call(
        scale,
        out_shape=(
            jax.ShapeDtypeStruct((6, rows, cols), f32),
            jax.ShapeDtypeStruct((1, 1), f32),
        ),
        in_specs=[whole] * 2,
        out_specs=(whole,) * 2,
        name="scale",
    )(image, sums)
    return mode, estimate[0, 0]


def solution(mesh):
    placed = (P(None, "gx", "gy"), P(None, "gx", "gy"), P("gx", "gy"))
    return jax.shard_map(
        on_device, mesh=mesh, in_specs=placed, out_specs=(P(None, "gx", "gy"), P()), check_vma=False
    )
```

```python
import jax
import jax.numpy as jnp
from jax import lax
from jax.experimental import pallas as pl
from jax.experimental.pallas import tpu as pltpu
from jax.sharding import PartitionSpec as P

TILE = 16
ITERS = 4
LANES = 128
SUB = 8
STRIP = 16
PAD = 24
epsilon = 1e-06
f32 = jnp.float32
bf16 = jnp.bfloat16
FIELD_SCALE = (18.0, 18.0, 1.0, 18.0, 18.0, 1.0)
TENSOR_SCALE = (
    1.0 / 576.0,
    1.0 / 576.0,
    1.0 / (576.0 * 324.0),
    1.0 / 576.0,
    1.0 / (576.0 * 18.0),
    1.0 / (576.0 * 18.0),
)
BELOW = 324.0


def lane_index(rows):
    return lax.broadcasted_iota(jnp.int32, (rows, LANES), 1)


def shifted(value, amount):
    amount = amount % LANES
    return value if amount == 0 else pltpu.roll(value, amount, 1)


def heavy_cells(class_map, rows, cols):
    tiles_x, tiles_y = class_map.shape
    row_of = lax.broadcasted_iota(jnp.int32, (rows, tiles_x), 0) // TILE
    row_pick = (row_of == lax.broadcasted_iota(jnp.int32, (rows, tiles_x), 1)).astype(f32)
    col_of = lax.broadcasted_iota(jnp.int32, (tiles_y, cols), 1) // TILE
    col_pick = (col_of == lax.broadcasted_iota(jnp.int32, (tiles_y, cols), 0)).astype(f32)
    spread = jnp.dot(row_pick, class_map.astype(f32), preferred_element_type=f32)
    return jnp.dot(spread, col_pick, preferred_element_type=f32)


def pack_kernel(start, tensor, class_map, left, right, top, bottom, mask):
    rows, cols = start.shape[1:]
    mask[...] = heavy_cells(class_map[...], rows, cols)

    def source(index, first):
        if index < 6:
            return start[index, pl.ds(first, STRIP), :].astype(f32)
        value = tensor[index - 6, pl.ds(first, STRIP), :].astype(f32)
        if index >= 9:
            value = value * mask[pl.ds(first, STRIP), :]
        return value

    lanes = lane_index(STRIP)
    per = LANES // STRIP

    def block(step, carry):
        first = pl.multiple_of(step * STRIP, STRIP)
        for group in range(2):
            low_part = jnp.zeros((STRIP, LANES), f32)
            high_part = jnp.zeros((STRIP, LANES), f32)
            for index in range(group * per, min(12, (group + 1) * per)):
                value = source(index, first)
                ends = jnp.where(lanes < LANES // 2, value[:, :LANES], value[:, LANES:])
                slot = index % per
                ends = shifted(ends, STRIP * slot)
                low_part = jnp.where(lanes // STRIP == slot, ends, low_part)
                high_part = jnp.where(lanes // STRIP == (slot - 1) % per, ends, high_part)
            left[pl.ds(first, STRIP), group * LANES : (group + 1) * LANES] = low_part.astype(bf16)
            right[pl.ds(first, STRIP), group * LANES : (group + 1) * LANES] = high_part.astype(bf16)
        return carry

    lax.fori_loop(0, rows // STRIP, block, 0)
    for index in range(12):
        top[index * STRIP : (index + 1) * STRIP, :] = source(index, 0).astype(bf16)
        bottom[index * STRIP : (index + 1) * STRIP, :] = source(index, rows - STRIP).astype(bf16)


def along(minus, centre, plus, plus2):
    return 27.0 * (plus - centre) - (plus2 - minus)


def main_kernel(
    start, tensor, class_map, left, right, above, below, out, sums, field, flux, coef, mask, keep, keep2, inner
):
    rows, cols = start.shape[1:]
    tiles = field.shape[0]
    per = LANES // STRIP
    bounds = (0, 3 * LANES // 4, cols - 3 * LANES // 4, cols)
    row_base = lax.axis_index("gx") * rows
    col_base = lax.axis_index("gy") * cols
    total_rows = rows * lax.axis_size("gx")
    total_cols = cols * lax.axis_size("gy")
    mask[...] = heavy_cells(class_map[...], rows, cols)
    deep = field.shape[2]

    for tile in range(tiles):
        r = lax.broadcasted_iota(jnp.int32, (deep, LANES), 0) - PAD
        c = lax.broadcasted_iota(jnp.int32, (deep, LANES), 1)
        if tile == 0:
            c = jnp.where(c < LANES - STRIP, c, c - LANES)
        elif tile == 1:
            c = jnp.where(c < LANES // 2, c + LANES, c)
        else:
            c = jnp.where(c < STRIP, c + cols, c + LANES)
        gr, gc = r + row_base, c + col_base
        good = (gr >= 0) & (gr < total_rows) & (gc >= 0) & (gc < total_cols)
        keep[tile] = jnp.where(good, 1.0, 0.0)
        keep2[tile] = jnp.where(good, BELOW, 0.0)
        mine = (r >= 0) & (r < rows) & (c >= bounds[tile]) & (c < bounds[tile + 1])
        inner[tile] = jnp.where(mine, 1.0, 0.0)
        edge = jnp.zeros((SUB, LANES), f32)
        for index in range(6):
            for first in (0, deep - SUB):
                field[tile, index, first : first + SUB, :] = edge
                flux[tile, index, first : first + SUB, :] = edge

    lanes = lane_index(STRIP)

    def place(index, first, value, strips):
        target = field if index < 6 else coef
        which = index if index < 6 else index - 6
        factor = FIELD_SCALE[index] if index < 6 else TENSOR_SCALE[index - 6]
        slot = index % per
        ends = shifted(strips[index // per][slot % 2], -STRIP * slot)
        one, two = value[:, :LANES], value[:, LANES:]
        if factor != 1.0:
            one, two, ends = one * factor, two * factor, ends * factor
        target[0, which, pl.ds(first, STRIP), :] = jnp.where(lanes < LANES - STRIP, one, ends)
        target[1, which, pl.ds(first, STRIP), :] = jnp.where(lanes < LANES // 2, two, one)
        target[2, which, pl.ds(first, STRIP), :] = jnp.where(lanes < STRIP, ends, two)

    def merged(low_strip, high_strip):
        odd = (lanes // STRIP) % 2 == 1
        pairs = []
        for group in range(2):
            low = low_strip[:, group * LANES : (group + 1) * LANES]
            high = high_strip[:, group * LANES : (group + 1) * LANES]
            pairs.append((jnp.where(odd, low, high), jnp.where(odd, high, low)))
        return pairs

    def assemble(step, carry):
        first = pl.multiple_of(step * STRIP, STRIP)
        strips = merged(left[pl.ds(first, STRIP), :].astype(f32), right[pl.ds(first, STRIP), :].astype(f32))
        for index in range(12):
            if index < 6:
                value = start[index, pl.ds(first, STRIP), :].astype(f32)
            else:
                value = tensor[index - 6, pl.ds(first, STRIP), :].astype(f32)
                if index >= 9:
                    value = value * mask[pl.ds(first, STRIP), :]
            place(index, PAD + first, value, strips)
        return carry

    lax.fori_loop(0, rows // STRIP, assemble, 0)
    for strip, first in ((above, PAD - STRIP), (below, PAD + rows)):
        strips = merged(
            strip[12 * STRIP : 13 * STRIP, :].astype(f32), strip[13 * STRIP : 14 * STRIP, :].astype(f32)
        )
        for index in range(12):
            place(index, first, strip[index * STRIP : (index + 1) * STRIP, :].astype(f32), strips)

    def load(ref, tile, index, first, offset):
        return ref[tile, index, pl.ds(first + offset, SUB), :]

    def curl(ref, tile, first, back):
        out_parts = []
        centre = [load(ref, tile, index, first, 0) for index in range(6)]

        def across(value):
            if back:
                other = shifted(value, 2)
                return 27.0 * value + other, -shifted(27.0 * other + value, -1)
            other = shifted(value, -2)
            return -(27.0 * value + other), shifted(27.0 * other + value, 1)

        def down(index):
            cells = [
                centre[index] if step == 0 else load(ref, tile, index, first, step)
                for step in range(-1 - back, 3 - back)
            ]
            return along(*cells)

        for part in range(2):
            x, y, z = centre[3 * part : 3 * part + 3]
            ox, oy = centre[3 - 3 * part], centre[4 - 3 * part]
            xn, xf = across(x)
            zn, zf = across(z)
            dxz = down(3 * part + 2)
            dxy = down(3 * part + 1)
            hz = (dxy - xn) - xf
            if part == 0:
                out_parts.append(((zn + oy) + zf, -(ox + dxz), hz))
            else:
                out_parts.append(((zn - oy) + zf, ox - dxz, hz))
        return out_parts

    def contract(tile, first, parts):
        k = [load(coef, tile, index, first, 0) for index in range(6)]
        results = []
        for cx, cy, cz in parts:
            results.append(
                (
                    k[0] * cx + k[3] * cy + k[4] * cz,
                    k[3] * cx + k[1] * cy + k[5] * cz,
                    k[4] * cx + k[5] * cy + k[2] * cz,
                )
            )
        return results

    unroll = 24

    def over(span, body, carry):
        lo = (PAD + span[0]) // SUB * SUB
        hi = -(-(PAD + span[1]) // SUB) * SUB
        count = (hi - lo) // SUB

        def chunk(size, at, carry):
            for inside in range(size):
                carry = body(at + inside * SUB, carry)
            return carry

        whole = count // unroll

        def loop(step, carry):
            return chunk(unroll, pl.multiple_of(lo + step * (unroll * SUB), SUB), carry)

        carry = lax.fori_loop(0, whole, loop, carry)
        if count % unroll:
            carry = chunk(count % unroll, lo + whole * unroll * SUB, carry)
        return carry

    zero = jnp.zeros((SUB, LANES), f32)

    def run_tile(tile, totals):
        totals = list(totals)
        for turn in range(ITERS):
            reach = 3 * (ITERS - 1 - turn)

            def first_half(first, carry):
                m, m2 = keep[tile, pl.ds(first, SUB), :], keep2[tile, pl.ds(first, SUB), :]
                for part, (hx, hy, hz) in enumerate(curl(field, tile, first, 0)):
                    flux[tile, 3 * part, pl.ds(first, SUB), :] = hx * m2
                    flux[tile, 3 * part + 1, pl.ds(first, SUB), :] = hy * m2
                    flux[tile, 3 * part + 2, pl.ds(first, SUB), :] = hz * m
                return carry

            over((-3 - reach, rows + 3 + reach), first_half, 0)

            def second_half(first, carry):
                flat, upright = carry
                results = contract(tile, first, curl(flux, tile, first, 1))
                for part, triple in enumerate(results):
                    for axis in range(3):
                        field[tile, 3 * part + axis, pl.ds(first, SUB), :] = triple[axis]
                (ax, ay, az), (bx, by, bz) = results
                own = inner[tile, pl.ds(first, SUB), :]
                flat = flat + own * ((ax * ax + ay * ay) + (bx * bx + by * by))
                upright = upright + own * (az * az + bz * bz)
                return flat, upright

            flat, upright = over((-1 - reach, rows + 2 + reach), second_half, (zero, zero))
            totals[turn] = totals[turn] + (flat * (1.0 / 324.0) + upright)

        def weigh(first, carry):
            e = [load(field, tile, index, first, 0) for index in range(6)]
            parts = contract(tile, first, ((e[0], e[1], BELOW * e[2]), (e[3], e[4], BELOW * e[5])))
            for part, triple in enumerate(parts):
                for axis in range(3):
                    flux[tile, 3 * part + axis, pl.ds(first, SUB), :] = triple[axis]
            return carry

        over((-1, rows + 2), weigh, 0)

        def pair(first, carry):
            flat, upright = carry
            one = curl(field, tile, first, 0)
            two = curl(flux, tile, first, 0)
            own = inner[tile, pl.ds(first, SUB), :]
            flat = flat + own * (
                (one[0][0] * two[0][0] + one[0][1] * two[0][1]) + (one[1][0] * two[1][0] + one[1][1] * two[1][1])
            )
            upright = upright + own * (one[0][2] * two[0][2] + one[1][2] * two[1][2])
            return flat, upright

        flat, upright = over((0, rows), pair, (zero, zero))
        totals[ITERS] = totals[ITERS] + (flat + upright * (1.0 / 324.0))
        return tuple(totals)

    totals = lax.fori_loop(0, tiles, run_tile, (zero,) * (ITERS + 1))

    line_lanes = lax.broadcasted_iota(jnp.int32, (1, LANES), 1)
    line = jnp.zeros((1, LANES), f32)
    for number, total in enumerate(totals):
        amount = jnp.sum(jnp.sum(total, axis=0, keepdims=True), axis=1, keepdims=True)
        line = jnp.where(line_lanes == number, amount, line)
    sums[...] = jnp.broadcast_to(line, sums.shape)

    sub_lanes = lane_index(SUB)

    def collect(step, carry):
        first = pl.multiple_of(step * SUB, SUB)
        for index in range(6):
            parts = [field[tile, index, pl.ds(PAD + first, SUB), :] for tile in range(tiles)]
            out[index, pl.ds(first, SUB), :LANES] = jnp.where(sub_lanes < bounds[1], parts[0], parts[1])
            out[index, pl.ds(first, SUB), LANES:] = jnp.where(sub_lanes < bounds[2] - LANES, parts[1], parts[2])
        return carry

    lax.fori_loop(0, rows // SUB, collect, 0)


def scale_kernel(cell_count, field, sums, out, estimate):
    totals = jnp.sum(sums[...], axis=0, keepdims=True)
    picks = [totals[:, number : number + 1] for number in range(ITERS + 1)]
    factor = jnp.ones((1, 1), f32)
    for number in range(ITERS):
        square_sum = factor * factor * picks[number]
        factor = factor * lax.rsqrt(square_sum / cell_count + epsilon)
    estimate[...] = picks[ITERS] / picks[ITERS - 1]
    flat = factor * (1.0 / 18.0)
    for index in range(6):
        out[index] = field[index] * (factor if index % 3 == 2 else flat)


def on_device(start_field, tensor, class_map):
    rows, cols = start_field.shape[1:]
    devices = lax.axis_size("gx") * lax.axis_size("gy")
    cell_count = rows * cols * devices
    if cols != 2 * LANES or rows % STRIP:
        raise ValueError("block shape")
    tiles = 3
    whole = pl.BlockSpec(memory_space=pltpu.VMEM)
    strip_rows = 12 * STRIP
    left, right, top, bottom = pl.pallas_call(
        pack_kernel,
        out_shape=(
            jax.ShapeDtypeStruct((rows, 2 * LANES), bf16),
            jax.ShapeDtypeStruct((rows, 2 * LANES), bf16),
            jax.ShapeDtypeStruct((strip_rows, cols), bf16),
            jax.ShapeDtypeStruct((strip_rows, cols), bf16),
        ),
        in_specs=[whole] * 3,
        out_specs=(whole,) * 4,
        scratch_shapes=[pltpu.VMEM((rows, cols), f32)],
        name="pack",
    )(start_field, tensor, class_map)

    def both(low_going, high_going, axis):
        count = lax.axis_size(axis)
        up = [(i, i + 1) for i in range(count - 1)]
        down = [(j, i) for i, j in up]
        return lax.ppermute(high_going, axis, up), lax.ppermute(low_going, axis, down)

    from_left, from_right = both(left, right, "gy")
    top = jnp.concatenate([top, from_left[:STRIP], from_right[:STRIP]])
    bottom = jnp.concatenate([bottom, from_left[-STRIP:], from_right[-STRIP:]])
    above, below = both(top, bottom, "gx")
    deep = rows + 2 * PAD
    plane = pltpu.VMEM((tiles, deep, LANES), f32)
    stack = pltpu.VMEM((tiles, 6, deep, LANES), f32)

    image, sums = pl.pallas_call(
        main_kernel,
        out_shape=(
            jax.ShapeDtypeStruct((6, rows, cols), f32),
            jax.ShapeDtypeStruct((devices, LANES), f32),
        ),
        in_specs=[whole] * 7,
        out_specs=(whole,) * 2,
        scratch_shapes=[stack, stack, stack, pltpu.VMEM((rows, cols), f32), plane, plane, plane],
        name="products",
    )(start_field, tensor, class_map, from_left, from_right, above, below)
    sums = lax.all_to_all(sums, ("gx", "gy"), 0, 0, tiled=True)

    def scale(*refs):
        scale_kernel(float(cell_count), *refs)

    mode, estimate = pl.pallas_call(
        scale,
        out_shape=(
            jax.ShapeDtypeStruct((6, rows, cols), f32),
            jax.ShapeDtypeStruct((1, 1), f32),
        ),
        in_specs=[whole] * 2,
        out_specs=(whole,) * 2,
        name="scale",
    )(image, sums)
    return mode, estimate[0, 0]


def solution(mesh):
    placed = (P(None, "gx", "gy"), P(None, "gx", "gy"), P("gx", "gy"))
    return jax.shard_map(
        on_device, mesh=mesh, in_specs=placed, out_specs=(P(None, "gx", "gy"), P()), check_vma=False
    )
```

```python
import jax
import jax.numpy as jnp
from jax import lax
from jax.experimental import pallas as pl
from jax.experimental.pallas import tpu as pltpu
from jax.sharding import PartitionSpec as P

TILE = 16
ITERS = 4
LANES = 128
SUB = 8
STRIP = 16
PAD = 24
epsilon = 1e-06
f32 = jnp.float32
bf16 = jnp.bfloat16
FIELD_SCALE = (18.0, 18.0, 1.0, 18.0, 18.0, 1.0)
TENSOR_SCALE = (
    1.0 / 576.0,
    1.0 / 576.0,
    1.0 / (576.0 * 324.0),
    1.0 / 576.0,
    1.0 / (576.0 * 18.0),
    1.0 / (576.0 * 18.0),
)
BELOW = 324.0
LAG = 8


def lane_index(rows):
    return lax.broadcasted_iota(jnp.int32, (rows, LANES), 1)


def shifted(value, amount):
    amount = amount % LANES
    return value if amount == 0 else pltpu.roll(value, amount, 1)


def heavy_cells(class_map, rows, cols):
    tiles_x, tiles_y = class_map.shape
    row_of = lax.broadcasted_iota(jnp.int32, (rows, tiles_x), 0) // TILE
    row_pick = (row_of == lax.broadcasted_iota(jnp.int32, (rows, tiles_x), 1)).astype(f32)
    col_of = lax.broadcasted_iota(jnp.int32, (tiles_y, cols), 1) // TILE
    col_pick = (col_of == lax.broadcasted_iota(jnp.int32, (tiles_y, cols), 0)).astype(f32)
    spread = jnp.dot(row_pick, class_map.astype(f32), preferred_element_type=f32)
    return jnp.dot(spread, col_pick, preferred_element_type=f32)


def is_even(axis):
    return lax.rem(lax.axis_index(axis), 2) == 0


def pack_kernel(start, tensor, class_map, near_cols, far_cols, near_rows, far_rows, mask):
    rows, cols = start.shape[1:]
    even_col, even_row = is_even("gy"), is_even("gx")
    mask[...] = heavy_cells(class_map[...], rows, cols)

    def source(index, first):
        if index < 6:
            return start[index, pl.ds(first, STRIP), :].astype(f32)
        value = tensor[index - 6, pl.ds(first, STRIP), :].astype(f32)
        if index >= 9:
            value = value * mask[pl.ds(first, STRIP), :]
        return value

    lanes = lane_index(STRIP)
    per = LANES // STRIP

    def block(step, carry):
        first = pl.multiple_of(step * STRIP, STRIP)
        for group in range(2):
            low_part = jnp.zeros((STRIP, LANES), f32)
            high_part = jnp.zeros((STRIP, LANES), f32)
            for index in range(group * per, min(12, (group + 1) * per)):
                value = source(index, first)
                ends = jnp.where(lanes < LANES // 2, value[:, :LANES], value[:, LANES:])
                slot = index % per
                ends = shifted(ends, STRIP * slot)
                low_part = jnp.where(lanes // STRIP == slot, ends, low_part)
                high_part = jnp.where(lanes // STRIP == (slot - 1) % per, ends, high_part)
            span = slice(group * LANES, (group + 1) * LANES)
            near_cols[pl.ds(first, STRIP), span] = jnp.where(even_col, high_part, low_part).astype(bf16)
            far_cols[pl.ds(first, STRIP), span] = jnp.where(even_col, low_part, high_part).astype(bf16)
        return carry

    lax.fori_loop(0, rows // STRIP, block, 0)
    for index in range(12):
        top, bottom = source(index, 0), source(index, rows - STRIP)
        span = slice(index * STRIP, (index + 1) * STRIP)
        near_rows[span, :] = jnp.where(even_row, bottom, top).astype(bf16)
        far_rows[span, :] = jnp.where(even_row, top, bottom).astype(bf16)


def main_kernel(
    start, tensor, class_map, near_cols, far_cols, near_rows, far_rows, out, sums,
    field, flux, coef, mask, keep, keep2, inner, image, done
):
    rows, cols = start.shape[1:]
    tiles = field.shape[0]
    per = LANES // STRIP
    bounds = (0, 3 * LANES // 4, cols - 3 * LANES // 4, cols)
    row_base = lax.axis_index("gx") * rows
    col_base = lax.axis_index("gy") * cols
    total_rows = rows * lax.axis_size("gx")
    total_cols = cols * lax.axis_size("gy")
    mask[...] = heavy_cells(class_map[...], rows, cols)
    deep = field.shape[2]

    for tile in range(tiles):
        r = lax.broadcasted_iota(jnp.int32, (deep, LANES), 0) - PAD
        c = lax.broadcasted_iota(jnp.int32, (deep, LANES), 1)
        if tile == 0:
            c = jnp.where(c < LANES - STRIP, c, c - LANES)
        elif tile == 1:
            c = jnp.where(c < LANES // 2, c + LANES, c)
        else:
            c = jnp.where(c < STRIP, c + cols, c + LANES)
        gr, gc = r + row_base, c + col_base
        good = (gr >= 0) & (gr < total_rows) & (gc >= 0) & (gc < total_cols)
        keep[tile] = jnp.where(good, 1.0, 0.0)
        keep2[tile] = jnp.where(good, BELOW, 0.0)
        c = c[:SUB]
        inner[tile] = jnp.where((c >= bounds[tile]) & (c < bounds[tile + 1]), 1.0, 0.0)
        edge = jnp.zeros((SUB, LANES), f32)
        for index in range(6):
            for first in (0, deep - SUB):
                field[tile, index, first : first + SUB, :] = edge
                flux[tile, index, first : first + SUB, :] = edge

    lanes = lane_index(STRIP)

    def place(index, first, value, strips):
        target = field if index < 6 else coef
        which = index if index < 6 else index - 6
        factor = FIELD_SCALE[index] if index < 6 else TENSOR_SCALE[index - 6]
        slot = index % per
        ends = shifted(strips[index // per][slot % 2], -STRIP * slot)
        one, two = value[:, :LANES], value[:, LANES:]
        if factor != 1.0:
            one, two, ends = one * factor, two * factor, ends * factor
        target[0, which, pl.ds(first, STRIP), :] = jnp.where(lanes < LANES - STRIP, one, ends)
        target[1, which, pl.ds(first, STRIP), :] = jnp.where(lanes < LANES // 2, two, one)
        target[2, which, pl.ds(first, STRIP), :] = jnp.where(lanes < STRIP, ends, two)

    def merged(low_strip, high_strip):
        odd = (lanes // STRIP) % 2 == 1
        pairs = []
        for group in range(2):
            low = low_strip[:, group * LANES : (group + 1) * LANES]
            high = high_strip[:, group * LANES : (group + 1) * LANES]
            pairs.append((jnp.where(odd, low, high), jnp.where(odd, high, low)))
        return pairs

    even_col, even_row = is_even("gy"), is_even("gx")

    def sides(near, far):
        return merged(jnp.where(even_col, far, near), jnp.where(even_col, near, far))

    def assemble(step, carry):
        first = pl.multiple_of(step * STRIP, STRIP)
        strips = sides(near_cols[pl.ds(first, STRIP), :].astype(f32), far_cols[pl.ds(first, STRIP), :].astype(f32))
        for index in range(12):
            if index < 6:
                value = start[index, pl.ds(first, STRIP), :].astype(f32)
            else:
                value = tensor[index - 6, pl.ds(first, STRIP), :].astype(f32)
                if index >= 9:
                    value = value * mask[pl.ds(first, STRIP), :]
            place(index, PAD + first, value, strips)
        return carry

    lax.fori_loop(0, rows // STRIP, assemble, 0)
    for upper, first in ((True, PAD - STRIP), (False, PAD + rows)):
        def rows_of(at, upper=upper):
            near, far = near_rows[at : at + STRIP, :].astype(f32), far_rows[at : at + STRIP, :].astype(f32)
            return jnp.where(even_row, far, near) if upper else jnp.where(even_row, near, far)

        corner = (12 + (1 if upper else 0)) * STRIP
        strips = sides(rows_of(corner), rows_of(corner + 2 * STRIP))
        for index in range(12):
            place(index, first, rows_of(index * STRIP), strips)

    def load(ref, tile, index, first, offset):
        return ref[tile, index, pl.ds(first + offset, SUB), :]

    def curl(ref, tile, first, back):
        wanted = (0, 2, 3, 5)
        turn, again = (2, -1) if back else (-2, 1)
        others = {index: shifted(load(ref, tile, index, first, 0), turn) for index in wanted}
        yield None
        near, far = {}, {}
        for index in wanted:
            value, other = load(ref, tile, index, first, 0), others[index]
            near[index] = 27.0 * value + other
            far[index] = shifted(27.0 * other + value, again)
        yield None
        out_parts = []
        for part in range(2):
            xi, yi, zi = 3 * part, 3 * part + 1, 3 * part + 2
            ox, oy = load(ref, tile, 3 - xi, first, 0), load(ref, tile, 4 - xi, first, 0)

            def down(index):
                cells = [load(ref, tile, index, first, step) for step in range(-1 - back, 3 - back)]
                return 27.0 * (cells[2] - cells[1]), cells[3] - cells[0]

            gap, wide = down(zi)
            lean, broad = down(yi)
            hy = (wide - gap) - ox if part == 0 else (wide - gap) + ox
            if back:
                across = near[zi] - far[zi]
                hz = ((lean - broad) - near[xi]) + far[xi]
            else:
                across = far[zi] - near[zi]
                hz = ((lean - broad) + near[xi]) - far[xi]
            hx = across + oy if part == 0 else across - oy
            out_parts.append((hx, hy, hz))
        yield out_parts

    def contract(tile, first, parts):
        k = [load(coef, tile, index, first, 0) for index in range(6)]
        results = []
        for cx, cy, cz in parts:
            results.append(
                (
                    k[0] * cx + k[3] * cy + k[4] * cz,
                    k[3] * cx + k[1] * cy + k[5] * cz,
                    k[4] * cx + k[5] * cy + k[2] * cz,
                )
            )
        return results

    zero = jnp.zeros((SUB, LANES), f32)

    def blocks(low, high):
        return range((PAD + low) // SUB * SUB, -(-(PAD + high) // SUB) * SUB, SUB)

    def staged(jobs):
        jobs = list(jobs)
        stages = 3
        for step in range(len(jobs) + (stages - 1) * LAG):
            for stage in range(stages):
                number = step - stage * LAG
                if 0 <= number < len(jobs):
                    next(jobs[number], None)

    def first_half(tile, first):
        work = curl(field, tile, first, 0)
        next(work)
        yield
        next(work)
        yield
        m, m2 = keep[tile, pl.ds(first, SUB), :], keep2[tile, pl.ds(first, SUB), :]
        for part, (hx, hy, hz) in enumerate(next(work)):
            flux[tile, 3 * part, pl.ds(first, SUB), :] = hx * m2
            flux[tile, 3 * part + 1, pl.ds(first, SUB), :] = hy * m2
            flux[tile, 3 * part + 2, pl.ds(first, SUB), :] = hz * m
        yield

    def second_half(tile, first, totals):
        work = curl(flux, tile, first, 1)
        next(work)
        yield
        next(work)
        yield
        results = contract(tile, first, next(work))
        for part, triple in enumerate(results):
            for axis in range(3):
                field[tile, 3 * part + axis, pl.ds(first, SUB), :] = triple[axis]
        if PAD <= first < PAD + rows:
            (ax, ay, az), (bx, by, bz) = results
            flat, upright = totals[tile]
            flat = flat + ((ax * ax + ay * ay) + (bx * bx + by * by))
            totals[tile] = flat, upright + (az * az + bz * bz)
        yield

    def gathered(totals):
        amount = zero
        for tile in range(tiles):
            flat, upright = totals[tile]
            amount = amount + jnp.where(inner[tile] > 0.0, flat * (1.0 / 324.0) + upright, 0.0)
        return amount

    reach = 3 * (ITERS - 1)

    def product(number, norms):
        totals = [(zero, zero) for _ in range(tiles)]
        jobs = [first_half(tile, first) for tile in range(tiles) for first in blocks(-3 - reach, rows + 3 + reach)]
        jobs += [
            second_half(tile, first, totals)
            for tile in range(tiles)
            for first in blocks(-1 - reach, rows + 2 + reach)
        ]
        staged(jobs)
        amount = gathered(totals)
        return tuple(jnp.where(number == turn, amount, norms[turn]) for turn in range(ITERS))

    norms = lax.fori_loop(0, ITERS, product, (zero,) * ITERS)

    sub_lanes = lane_index(SUB)
    for first in range(0, rows, SUB):
        for index in range(6):
            parts = [field[tile, index, PAD + first : PAD + first + SUB, :] for tile in range(tiles)]
            image[index, first : first + SUB, :LANES] = jnp.where(sub_lanes < bounds[1], parts[0], parts[1])
            image[index, first : first + SUB, LANES:] = jnp.where(sub_lanes < bounds[2] - LANES, parts[1], parts[2])

    for tile in range(tiles):
        for first in blocks(-1, rows + 2):
            e = [load(field, tile, index, first, 0) for index in range(6)]
            parts = contract(tile, first, ((e[0], e[1], BELOW * e[2]), (e[3], e[4], BELOW * e[5])))
            for part, triple in enumerate(parts):
                for axis in range(3):
                    flux[tile, 3 * part + axis, pl.ds(first, SUB), :] = triple[axis]

    copy = pltpu.make_async_copy(image, out, done)
    copy.start()

    def pair(tile, first, totals):
        works = curl(field, tile, first, 0), curl(flux, tile, first, 0)
        for _ in range(2):
            for work in works:
                next(work)
            yield
        one, two = next(works[0]), next(works[1])
        flat, upright = totals[tile]
        flat = flat + ((one[0][0] * two[0][0] + one[0][1] * two[0][1]) + (one[1][0] * two[1][0] + one[1][1] * two[1][1]))
        totals[tile] = flat, upright + (one[0][2] * two[0][2] + one[1][2] * two[1][2])
        yield

    totals = [(zero, zero) for _ in range(tiles)]
    staged(pair(tile, first, totals) for tile in range(tiles) for first in blocks(0, rows))
    cross = zero
    for tile in range(tiles):
        flat, upright = totals[tile]
        cross = cross + jnp.where(inner[tile] > 0.0, flat + upright * (1.0 / 324.0), 0.0)
    totals = list(norms) + [cross]

    line_lanes = lax.broadcasted_iota(jnp.int32, (1, LANES), 1)
    line = jnp.zeros((1, LANES), f32)
    for number, total in enumerate(totals):
        amount = jnp.sum(jnp.sum(total, axis=0, keepdims=True), axis=1, keepdims=True)
        line = jnp.where(line_lanes == number, amount, line)
    sums[...] = jnp.broadcast_to(line, sums.shape)
    copy.wait()


def scale_kernel(cell_count, field, sums, out, estimate):
    totals = jnp.sum(sums[...], axis=0, keepdims=True)
    picks = [totals[:, number : number + 1] for number in range(ITERS + 1)]
    factor = jnp.ones((1, 1), f32)
    for number in range(ITERS):
        square_sum = factor * factor * picks[number]
        factor = factor * lax.rsqrt(square_sum / cell_count + epsilon)
    estimate[...] = picks[ITERS] / picks[ITERS - 1]
    flat = factor * (1.0 / 18.0)
    for index in range(6):
        out[index] = field[index] * (factor if index % 3 == 2 else flat)


def on_device(start_field, tensor, class_map):
    rows, cols = start_field.shape[1:]
    devices = lax.axis_size("gx") * lax.axis_size("gy")
    cell_count = rows * cols * devices
    if cols != 2 * LANES or rows % STRIP:
        raise ValueError("block shape")
    tiles = 3
    whole = pl.BlockSpec(memory_space=pltpu.VMEM)
    anywhere = pl.BlockSpec(memory_space=pl.ANY)
    strip_rows = 12 * STRIP
    near_cols, far_cols, near_rows, far_rows = pl.pallas_call(
        pack_kernel,
        out_shape=(
            jax.ShapeDtypeStruct((rows, 2 * LANES), bf16),
            jax.ShapeDtypeStruct((rows, 2 * LANES), bf16),
            jax.ShapeDtypeStruct((strip_rows, cols), bf16),
            jax.ShapeDtypeStruct((strip_rows, cols), bf16),
        ),
        in_specs=[whole] * 3,
        out_specs=(whole,) * 4,
        scratch_shapes=[pltpu.VMEM((rows, cols), f32)],
        name="pack",
    )(start_field, tensor, class_map)

    def traded(near, far, axis):
        count = lax.axis_size(axis)
        inward = [(i, i + 1) for i in range(1, count - 1, 2)]
        outward = [(i, i + 1) for i in range(0, count - 1, 2)]
        both = [pairs + [(j, i) for i, j in pairs] for pairs in (outward, inward)]
        far = lax.ppermute(far, axis, both[1])
        return lax.ppermute(near, axis, both[0]), far

    near_cols, far_cols = traded(near_cols, far_cols, "gy")
    corners = [near_cols[:STRIP], near_cols[-STRIP:], far_cols[:STRIP], far_cols[-STRIP:]]
    near_rows = jnp.concatenate([near_rows] + corners)
    far_rows = jnp.concatenate([far_rows] + corners)
    near_rows, far_rows = traded(near_rows, far_rows, "gx")
    deep = rows + 2 * PAD
    plane = pltpu.VMEM((tiles, deep, LANES), f32)
    stack = pltpu.VMEM((tiles, 6, deep, LANES), f32)

    image, sums = pl.pallas_call(
        main_kernel,
        out_shape=(
            jax.ShapeDtypeStruct((6, rows, cols), f32),
            jax.ShapeDtypeStruct((devices, LANES), f32),
        ),
        in_specs=[whole] * 7,
        out_specs=(anywhere, whole),
        scratch_shapes=[
            stack,
            stack,
            stack,
            pltpu.VMEM((rows, cols), f32),
            plane,
            plane,
            pltpu.VMEM((tiles, SUB, LANES), f32),
            pltpu.VMEM((6, rows, cols), f32),
            pltpu.SemaphoreType.DMA,
        ],
        compiler_params=pltpu.CompilerParams(),
        name="products",
    )(start_field, tensor, class_map, near_cols, far_cols, near_rows, far_rows)
    sums = lax.all_to_all(sums, ("gx", "gy"), 0, 0, tiled=True)

    def scale(*refs):
        scale_kernel(float(cell_count), *refs)

    mode, estimate = pl.pallas_call(
        scale,
        out_shape=(
            jax.ShapeDtypeStruct((6, rows, cols), f32),
            jax.ShapeDtypeStruct((1, 1), f32),
        ),
        in_specs=[whole] * 2,
        out_specs=(whole,) * 2,
        name="scale",
    )(image, sums)
    return mode, estimate[0, 0]


def solution(mesh):
    placed = (P(None, "gx", "gy"), P(None, "gx", "gy"), P("gx", "gy"))
    return jax.shard_map(
        on_device, mesh=mesh, in_specs=placed, out_specs=(P(None, "gx", "gy"), P()), check_vma=False
    )
```

```python
import jax
import jax.numpy as jnp
from jax import lax
from jax.experimental import pallas as pl
from jax.experimental.pallas import tpu as pltpu
from jax.sharding import PartitionSpec as P

TILE = 16
ITERS = 4
LANES = 128
SUB = 8
STRIP = 16
PAD = 24
epsilon = 1e-06
f32 = jnp.float32
bf16 = jnp.bfloat16
FIELD_SCALE = (18.0, 18.0, 1.0, 18.0, 18.0, 1.0)
TENSOR_SCALE = (
    1.0 / 576.0,
    1.0 / 576.0,
    1.0 / (576.0 * 324.0),
    1.0 / 576.0,
    1.0 / (576.0 * 18.0),
    1.0 / (576.0 * 18.0),
)
BELOW = 324.0
DEEP_FIELD = 14
DEEP_TENSOR = 11
LAG = 8
ROOM_SMALL = 8 << 20
ROOM_LARGE = 24 << 20


def row_place(index):
    if index < 6:
        return index * DEEP_FIELD, DEEP_FIELD
    return 6 * DEEP_FIELD + (index - 6) * DEEP_TENSOR, DEEP_TENSOR


def lane_index(rows):
    return lax.broadcasted_iota(jnp.int32, (rows, LANES), 1)


def shifted(value, amount):
    amount = amount % LANES
    return value if amount == 0 else pltpu.roll(value, amount, 1)


def heavy_cells(class_map, rows, cols):
    tiles_x, tiles_y = class_map.shape
    row_of = lax.broadcasted_iota(jnp.int32, (rows, tiles_x), 0) // TILE
    row_pick = (row_of == lax.broadcasted_iota(jnp.int32, (rows, tiles_x), 1)).astype(f32)
    col_of = lax.broadcasted_iota(jnp.int32, (tiles_y, cols), 1) // TILE
    col_pick = (col_of == lax.broadcasted_iota(jnp.int32, (tiles_y, cols), 0)).astype(f32)
    spread = jnp.dot(row_pick, class_map.astype(f32), preferred_element_type=f32)
    return jnp.dot(spread, col_pick, preferred_element_type=f32)


def is_even(axis):
    return lax.rem(lax.axis_index(axis), 2) == 0


def pack_kernel(
    start_in, tensor_in, class_in, near_cols, far_cols, near_rows, far_rows, start, tensor, class_map, mask, firsts, lasts, here
):
    copies = [
        pltpu.make_async_copy(source, target, here.at[number])
        for number, (source, target) in enumerate(((class_in, class_map), (tensor_in, tensor), (start_in, start)))
    ]
    for copy in copies:
        copy.start()
    rows, cols = start.shape[1:]
    even_col, even_row = is_even("gy"), is_even("gx")
    copies[0].wait()
    mask[...] = heavy_cells(class_map[...], rows, cols)
    copies[1].wait()
    copies[2].wait()

    def source(index, first):
        if index < 6:
            return start[index, first : first + STRIP, :].astype(f32)
        value = tensor[index - 6, first : first + STRIP, :].astype(f32)
        if index >= 9:
            value = value * mask[first : first + STRIP, :]
        return value

    lanes = lane_index(STRIP)
    per = LANES // STRIP

    def rotated(first):
        ends = []
        for index in range(12):
            value = source(index, first)
            value = jnp.where(lanes < LANES // 2, value[:, :LANES], value[:, LANES:])
            ends.append(shifted(value, STRIP * (index % per)))
        return ends

    def stored(first, ends):
        for group in range(2):
            low_part = jnp.zeros((STRIP, LANES), f32)
            high_part = jnp.zeros((STRIP, LANES), f32)
            for index in range(group * per, min(12, (group + 1) * per)):
                slot = index % per
                low_part = jnp.where(lanes // STRIP == slot, ends[index], low_part)
                high_part = jnp.where(lanes // STRIP == (slot - 1) % per, ends[index], high_part)
            span = slice(group * LANES, (group + 1) * LANES)
            near_cols[first : first + STRIP, span] = jnp.where(even_col, high_part, low_part).astype(bf16)
            far_cols[first : first + STRIP, span] = jnp.where(even_col, low_part, high_part).astype(bf16)

    places = list(range(0, rows, STRIP))
    waiting = [rotated(places[0])]
    for index in range(12):
        value = source(index, 0)
        at, _ = row_place(index)
        for piece in range(2):
            firsts[piece, at : at + STRIP, :] = value[:, piece * LANES : (piece + 1) * LANES]
    for index in reversed(range(12)):
        value = source(index, rows - STRIP)
        at, count = row_place(index)
        at = STRIP + at + count - STRIP
        for piece in range(2):
            lasts[piece, at : at + STRIP, :] = value[:, piece * LANES : (piece + 1) * LANES]
    for number, first in enumerate(places):
        if number + 1 < len(places):
            waiting.append(rotated(places[number + 1]))
        stored(first, waiting[number])
    for piece in range(2):
        span = slice(piece * LANES, (piece + 1) * LANES)
        top = firsts[piece, : near_rows.shape[0], :]
        bottom = lasts[piece, STRIP : STRIP + near_rows.shape[0], :]
        near_rows[:, span] = jnp.where(even_row, bottom, top).astype(bf16)
        far_rows[:, span] = jnp.where(even_row, top, bottom).astype(bf16)


def main_kernel(
    start, tensor, class_map, near_cols, far_cols, near_rows, far_rows, image, sums,
    field, flux, coef, mask, keep, keep2, inner, wide
):
    rows, cols = start.shape[1:]
    tiles = field.shape[0]
    per = LANES // STRIP
    bounds = (0, 3 * LANES // 4, cols - 3 * LANES // 4, cols)
    row_base = lax.axis_index("gx") * rows
    col_base = lax.axis_index("gy") * cols
    total_rows = rows * lax.axis_size("gx")
    total_cols = cols * lax.axis_size("gy")
    mask[...] = heavy_cells(class_map[...], rows, cols)
    deep = field.shape[2]

    for tile in range(tiles):
        r = lax.broadcasted_iota(jnp.int32, (deep, LANES), 0) - PAD
        c = lax.broadcasted_iota(jnp.int32, (deep, LANES), 1)
        if tile == 0:
            c = jnp.where(c < LANES - STRIP, c, c - LANES)
        elif tile == 1:
            c = jnp.where(c < LANES // 2, c + LANES, c)
        else:
            c = jnp.where(c < STRIP, c + cols, c + LANES)
        gr, gc = r + row_base, c + col_base
        good = (gr >= 0) & (gr < total_rows) & (gc >= 0) & (gc < total_cols)
        keep[tile] = jnp.where(good, 1.0, 0.0)
        keep2[tile] = jnp.where(good, BELOW, 0.0)
        c = c[:SUB]
        inner[tile] = jnp.where((c >= bounds[tile]) & (c < bounds[tile + 1]), 1.0, 0.0)
        edge = jnp.zeros((SUB, LANES), f32)
        for index in range(6):
            for first in (0, deep - SUB):
                flux[tile, index, first : first + SUB, :] = edge
            for first in (0, SUB, PAD + rows + SUB, deep - SUB):
                field[tile, index, first : first + SUB, :] = edge
                coef[tile, index, first : first + SUB, :] = edge

    lanes = lane_index(STRIP)

    def turned(index, strips):
        slot = index % per
        return shifted(strips[index // per][slot % 2], -STRIP * slot)

    def place(index, first, one, two, ends):
        target = field if index < 6 else coef
        which = index if index < 6 else index - 6
        factor = FIELD_SCALE[index] if index < 6 else TENSOR_SCALE[index - 6]
        if factor != 1.0:
            one, two, ends = one * factor, two * factor, ends * factor
        count = one.shape[0]
        lane = lane_index(count)
        target[0, which, first : first + count, :] = jnp.where(lane < LANES - STRIP, one, ends)
        target[1, which, first : first + count, :] = jnp.where(lane < LANES // 2, two, one)
        target[2, which, first : first + count, :] = jnp.where(lane < STRIP, ends, two)

    def merged(low_strip, high_strip):
        odd = (lanes // STRIP) % 2 == 1
        pairs = []
        for group in range(2):
            low = low_strip[:, group * LANES : (group + 1) * LANES]
            high = high_strip[:, group * LANES : (group + 1) * LANES]
            pairs.append((jnp.where(odd, low, high), jnp.where(odd, high, low)))
        return pairs

    even_col, even_row = is_even("gy"), is_even("gx")

    def sides(near, far):
        return merged(jnp.where(even_col, far, near), jnp.where(even_col, near, far))

    def begun(first):
        strips = sides(
            near_cols[first : first + STRIP, :].astype(f32), far_cols[first : first + STRIP, :].astype(f32)
        )
        return [turned(index, strips) for index in range(12)]

    def ended(first, ends):
        for index in range(12):
            if index < 6:
                value = start[index, first : first + STRIP, :].astype(f32)
            else:
                value = tensor[index - 6, first : first + STRIP, :].astype(f32)
                if index >= 9:
                    value = value * mask[first : first + STRIP, :]
            place(index, PAD + first, value[:, :LANES], value[:, LANES:], ends[index])

    places = list(range(0, rows, STRIP))
    waiting = [begun(places[0])]
    for number, first in enumerate(places):
        if number + 1 < len(places):
            waiting.append(begun(places[number + 1]))
        ended(first, waiting[number])

    packed = near_rows.shape[0] - 4 * STRIP
    for upper, edge in ((True, PAD), (False, PAD + rows)):
        def rows_of(at, count, upper=upper):
            near, far = near_rows[at : at + count, :].astype(f32), far_rows[at : at + count, :].astype(f32)
            return jnp.where(even_row, far, near) if upper else jnp.where(even_row, near, far)

        corner = packed + (STRIP if upper else 0)
        strips = sides(rows_of(corner, STRIP), rows_of(corner + 2 * STRIP, STRIP))
        ends = [turned(index, strips) for index in range(12)]
        level = 0 if upper else 1
        value = rows_of(0, packed)
        for piece in range(2):
            wide[level, piece] = value[:, piece * LANES : (piece + 1) * LANES]
        for index in range(12):
            at, count = row_place(index)
            for begin in (0, count - SUB):
                row = begin + (STRIP - count if upper else 0)
                corner_ends = ends[index][row : row + SUB]
                first = edge + begin - (count if upper else 0)
                one, two = wide[level, 0, at + begin : at + begin + SUB, :], wide[level, 1, at + begin : at + begin + SUB, :]
                place(index, first, one, two, corner_ends)

    def load(ref, tile, index, first, offset):
        return ref[tile, index, pl.ds(first + offset, SUB), :]

    def curl(ref, tile, first, back):
        wanted = (0, 2, 3, 5)
        turn, again = (2, -1) if back else (-2, 1)
        others = {index: shifted(load(ref, tile, index, first, 0), turn) for index in wanted}
        yield None
        near, far = {}, {}
        for index in wanted:
            value, other = load(ref, tile, index, first, 0), others[index]
            near[index] = 27.0 * value + other
            far[index] = shifted(27.0 * other + value, again)
        yield None
        out_parts = []
        for part in range(2):
            xi, yi, zi = 3 * part, 3 * part + 1, 3 * part + 2
            ox, oy = load(ref, tile, 3 - xi, first, 0), load(ref, tile, 4 - xi, first, 0)

            def down(index):
                cells = [load(ref, tile, index, first, step) for step in range(-1 - back, 3 - back)]
                return 27.0 * (cells[2] - cells[1]), cells[3] - cells[0]

            gap, wide = down(zi)
            lean, broad = down(yi)
            hy = (wide - gap) - ox if part == 0 else (wide - gap) + ox
            if back:
                across = near[zi] - far[zi]
                hz = ((lean - broad) - near[xi]) + far[xi]
            else:
                across = far[zi] - near[zi]
                hz = ((lean - broad) + near[xi]) - far[xi]
            hx = across + oy if part == 0 else across - oy
            out_parts.append((hx, hy, hz))
        yield out_parts

    def contract(tile, first, parts):
        k = [load(coef, tile, index, first, 0) for index in range(6)]
        results = []
        for cx, cy, cz in parts:
            results.append(
                (
                    k[0] * cx + k[3] * cy + k[4] * cz,
                    k[3] * cx + k[1] * cy + k[5] * cz,
                    k[4] * cx + k[5] * cy + k[2] * cz,
                )
            )
        return results

    zero = jnp.zeros((SUB, LANES), f32)

    def blocks(low, high):
        return range((PAD + low) // SUB * SUB, -(-(PAD + high) // SUB) * SUB, SUB)

    def staged(jobs):
        jobs = list(jobs)
        stages = 3
        for step in range(len(jobs) + (stages - 1) * LAG):
            for stage in range(stages):
                number = step - stage * LAG
                if 0 <= number < len(jobs):
                    next(jobs[number], None)

    def first_half(tile, first):
        work = curl(field, tile, first, 0)
        next(work)
        yield
        next(work)
        yield
        m, m2 = keep[tile, pl.ds(first, SUB), :], keep2[tile, pl.ds(first, SUB), :]
        for part, (hx, hy, hz) in enumerate(next(work)):
            flux[tile, 3 * part, pl.ds(first, SUB), :] = hx * m2
            flux[tile, 3 * part + 1, pl.ds(first, SUB), :] = hy * m2
            flux[tile, 3 * part + 2, pl.ds(first, SUB), :] = hz * m
        yield

    def second_half(tile, first, totals):
        work = curl(flux, tile, first, 1)
        next(work)
        yield
        next(work)
        yield
        results = contract(tile, first, next(work))
        for part, triple in enumerate(results):
            for axis in range(3):
                field[tile, 3 * part + axis, pl.ds(first, SUB), :] = triple[axis]
        if PAD <= first < PAD + rows:
            (ax, ay, az), (bx, by, bz) = results
            flat, upright = totals[tile]
            flat = flat + ((ax * ax + ay * ay) + (bx * bx + by * by))
            totals[tile] = flat, upright + (az * az + bz * bz)
        yield

    def gathered(totals):
        amount = zero
        for tile in range(tiles):
            flat, upright = totals[tile]
            amount = amount + jnp.where(inner[tile] > 0.0, flat * (1.0 / 324.0) + upright, 0.0)
        return amount

    reach = 3 * (ITERS - 1)

    def product(number, norms):
        totals = [(zero, zero) for _ in range(tiles)]
        jobs = [first_half(tile, first) for tile in range(tiles) for first in blocks(-3 - reach, rows + 3 + reach)]
        jobs += [
            second_half(tile, first, totals)
            for tile in range(tiles)
            for first in blocks(-1 - reach, rows + 2 + reach)
        ]
        staged(jobs)
        amount = gathered(totals)
        return tuple(jnp.where(number == turn, amount, norms[turn]) for turn in range(ITERS))

    norms = lax.fori_loop(0, ITERS, product, (zero,) * ITERS)

    sub_lanes = lane_index(SUB)
    for first in range(0, rows, SUB):
        for index in range(6):
            parts = [field[tile, index, PAD + first : PAD + first + SUB, :] for tile in range(tiles)]
            image[index, first : first + SUB, :LANES] = jnp.where(sub_lanes < bounds[1], parts[0], parts[1])
            image[index, first : first + SUB, LANES:] = jnp.where(sub_lanes < bounds[2] - LANES, parts[1], parts[2])

    for tile in range(tiles):
        for first in blocks(-1, rows + 2):
            e = [load(field, tile, index, first, 0) for index in range(6)]
            parts = contract(tile, first, ((e[0], e[1], BELOW * e[2]), (e[3], e[4], BELOW * e[5])))
            for part, triple in enumerate(parts):
                for axis in range(3):
                    flux[tile, 3 * part + axis, pl.ds(first, SUB), :] = triple[axis]

    def pair(tile, first, totals):
        works = curl(field, tile, first, 0), curl(flux, tile, first, 0)
        for _ in range(2):
            for work in works:
                next(work)
            yield
        one, two = next(works[0]), next(works[1])
        flat, upright = totals[tile]
        flat = flat + ((one[0][0] * two[0][0] + one[0][1] * two[0][1]) + (one[1][0] * two[1][0] + one[1][1] * two[1][1]))
        totals[tile] = flat, upright + (one[0][2] * two[0][2] + one[1][2] * two[1][2])
        yield

    totals = [(zero, zero) for _ in range(tiles)]
    staged(pair(tile, first, totals) for tile in range(tiles) for first in blocks(0, rows))
    cross = zero
    for tile in range(tiles):
        flat, upright = totals[tile]
        cross = cross + jnp.where(inner[tile] > 0.0, flat + upright * (1.0 / 324.0), 0.0)
    totals = list(norms) + [cross]

    line_lanes = lax.broadcasted_iota(jnp.int32, (1, LANES), 1)
    line = jnp.zeros((1, LANES), f32)
    for number, total in enumerate(totals):
        amount = jnp.sum(jnp.sum(total, axis=0, keepdims=True), axis=1, keepdims=True)
        line = jnp.where(line_lanes == number, amount, line)
    sums[...] = jnp.broadcast_to(line, sums.shape)


def scale_kernel(cell_count, field, sums, out, estimate):
    totals = jnp.sum(sums[...], axis=0, keepdims=True)
    picks = [totals[:, number : number + 1] for number in range(ITERS + 1)]
    factor = jnp.ones((1, 1), f32)
    for number in range(ITERS):
        square_sum = factor * factor * picks[number]
        factor = factor * lax.rsqrt(square_sum / cell_count + epsilon)
    estimate[...] = picks[ITERS] / picks[ITERS - 1]
    flat = factor * (1.0 / 18.0)
    for index in range(6):
        out[index] = field[index] * (factor if index % 3 == 2 else flat)


def on_device(start_field, tensor, class_map):
    rows, cols = start_field.shape[1:]
    devices = lax.axis_size("gx") * lax.axis_size("gy")
    cell_count = rows * cols * devices
    if cols != 2 * LANES or rows % STRIP:
        raise ValueError("block shape")
    tiles = 3
    whole = pl.BlockSpec(memory_space=pltpu.VMEM)
    strip_rows = -(-6 * (DEEP_FIELD + DEEP_TENSOR) // SUB) * SUB
    anywhere = pl.BlockSpec(memory_space=pltpu.HBM)
    near_cols, far_cols, near_rows, far_rows = pl.pallas_call(
        pack_kernel,
        out_shape=(
            jax.ShapeDtypeStruct((rows, 2 * LANES), bf16),
            jax.ShapeDtypeStruct((rows, 2 * LANES), bf16),
            jax.ShapeDtypeStruct((strip_rows, cols), bf16),
            jax.ShapeDtypeStruct((strip_rows, cols), bf16),
        ),
        in_specs=[anywhere] * 3,
        out_specs=(whole,) * 4,
        scratch_shapes=[
            pltpu.VMEM(start_field.shape, bf16),
            pltpu.VMEM(tensor.shape, bf16),
            pltpu.VMEM(class_map.shape, jnp.int32),
            pltpu.VMEM((rows, cols), f32),
            pltpu.VMEM((2, strip_rows + 2 * STRIP, LANES), f32),
            pltpu.VMEM((2, strip_rows + 2 * STRIP, LANES), f32),
            pltpu.SemaphoreType.DMA((3,)),
        ],
        compiler_params=pltpu.CompilerParams(vmem_limit_bytes=ROOM_SMALL),
        name="pack",
    )(*(pltpu.with_memory_space_constraint(array, pltpu.HBM) for array in (start_field, tensor, class_map)))

    def traded(near, far, axis):
        count = lax.axis_size(axis)
        inward = [(i, i + 1) for i in range(1, count - 1, 2)]
        outward = [(i, i + 1) for i in range(0, count - 1, 2)]
        both = [pairs + [(j, i) for i, j in pairs] for pairs in (outward, inward)]
        far = lax.ppermute(far, axis, both[1])
        return lax.ppermute(near, axis, both[0]), far

    near_cols, far_cols = traded(near_cols, far_cols, "gy")
    corners = [near_cols[:STRIP], near_cols[-STRIP:], far_cols[:STRIP], far_cols[-STRIP:]]
    near_rows = jnp.concatenate([near_rows] + corners)
    far_rows = jnp.concatenate([far_rows] + corners)
    near_rows, far_rows = traded(near_rows, far_rows, "gx")
    deep = rows + 2 * PAD
    plane = pltpu.VMEM((tiles, deep, LANES), f32)
    stack = pltpu.VMEM((tiles, 6, deep, LANES), f32)

    image, sums = pl.pallas_call(
        main_kernel,
        out_shape=(
            jax.ShapeDtypeStruct((6, rows, cols), f32),
            jax.ShapeDtypeStruct((devices, LANES), f32),
        ),
        in_specs=[whole] * 7,
        out_specs=(whole,) * 2,
        scratch_shapes=[
            stack,
            stack,
            stack,
            pltpu.VMEM((rows, cols), f32),
            plane,
            plane,
            pltpu.VMEM((tiles, SUB, LANES), f32),
            pltpu.VMEM((2, 2, strip_rows, LANES), f32),
        ],
        compiler_params=pltpu.CompilerParams(
            vmem_limit_bytes=ROOM_LARGE
        ),
        name="products",
    )(start_field, tensor, class_map, near_cols, far_cols, near_rows, far_rows)
    sums = lax.all_to_all(sums, ("gx", "gy"), 0, 0, tiled=True)

    def scale(*refs):
        scale_kernel(float(cell_count), *refs)

    mode, estimate = pl.pallas_call(
        scale,
        out_shape=(
            jax.ShapeDtypeStruct((6, rows, cols), f32),
            jax.ShapeDtypeStruct((1, 1), f32),
        ),
        in_specs=[whole] * 2,
        out_specs=(whole,) * 2,
        compiler_params=pltpu.CompilerParams(vmem_limit_bytes=ROOM_SMALL),
        name="scale",
    )(image, sums)
    return mode, estimate[0, 0]


def solution(mesh):
    placed = (P(None, "gx", "gy"), P(None, "gx", "gy"), P("gx", "gy"))
    return jax.shard_map(
        on_device, mesh=mesh, in_specs=placed, out_specs=(P(None, "gx", "gy"), P()), check_vma=False
    )
```

```python
import jax
import jax.numpy as jnp
from jax import lax
from jax.experimental import pallas as pl
from jax.experimental.pallas import tpu as pltpu
from jax.sharding import PartitionSpec as P

TILE = 16
ITERS = 4
LANES = 128
SUB = 8
STRIP = 16
PAD = 24
epsilon = 1e-06
f32 = jnp.float32
bf16 = jnp.bfloat16
FIELD_SCALE = (18.0, 18.0, 1.0, 18.0, 18.0, 1.0)
TENSOR_SCALE = (
    1.0 / 576.0,
    1.0 / 576.0,
    1.0 / (576.0 * 324.0),
    1.0 / 576.0,
    1.0 / (576.0 * 18.0),
    1.0 / (576.0 * 18.0),
)
BELOW = 324.0
DEEP_FIELD = 14
DEEP_TENSOR = 11
LAG = 10
ROOM_SMALL = 8 << 20
ROOM_LARGE = 24 << 20


def row_place(index):
    if index < 6:
        return index * DEEP_FIELD, DEEP_FIELD
    return 6 * DEEP_FIELD + (index - 6) * DEEP_TENSOR, DEEP_TENSOR


def lane_index(rows):
    return lax.broadcasted_iota(jnp.int32, (rows, LANES), 1)


def shifted(value, amount):
    amount = amount % LANES
    return value if amount == 0 else pltpu.roll(value, amount, 1)


def heavy_cells(class_map, rows, cols):
    tiles_x, tiles_y = class_map.shape
    row_of = lax.broadcasted_iota(jnp.int32, (rows, tiles_x), 0) // TILE
    row_pick = (row_of == lax.broadcasted_iota(jnp.int32, (rows, tiles_x), 1)).astype(f32)
    col_of = lax.broadcasted_iota(jnp.int32, (tiles_y, cols), 1) // TILE
    col_pick = (col_of == lax.broadcasted_iota(jnp.int32, (tiles_y, cols), 0)).astype(f32)
    spread = jnp.dot(row_pick, class_map.astype(f32), preferred_element_type=f32)
    return jnp.dot(spread, col_pick, preferred_element_type=f32)


def tile_columns(tile, cols, count):
    c = lane_index(count)
    if tile == 0:
        return jnp.where(c < LANES - STRIP, c, c - LANES)
    if tile == 1:
        return jnp.where(c < LANES // 2, c + LANES, c)
    return jnp.where(c < STRIP, c + cols, c + LANES)


def is_even(axis):
    return lax.rem(lax.axis_index(axis), 2) == 0


def pack_kernel(
    start_in, tensor_in, class_in, near_cols, far_cols, near_rows, far_rows, start, tensor, mask, class_map, firsts, lasts, here
):
    copies = [
        pltpu.make_async_copy(source, target, here.at[number])
        for number, (source, target) in enumerate(((class_in, class_map), (tensor_in, tensor), (start_in, start)))
    ]
    for copy in copies:
        copy.start()
    rows, cols = start.shape[1:]
    even_col, even_row = is_even("gy"), is_even("gx")
    copies[0].wait()
    mask[...] = heavy_cells(class_map[...], rows, cols)
    copies[1].wait()
    copies[2].wait()

    def source(index, first):
        if index < 6:
            return start[index, first : first + STRIP, :].astype(f32)
        value = tensor[index - 6, first : first + STRIP, :].astype(f32)
        if index >= 9:
            value = value * mask[first : first + STRIP, :]
        return value

    lanes = lane_index(STRIP)
    per = LANES // STRIP

    def rotated(first):
        ends = []
        for index in range(12):
            value = source(index, first)
            value = jnp.where(lanes < LANES // 2, value[:, :LANES], value[:, LANES:])
            ends.append(shifted(value, STRIP * (index % per)))
        return ends

    def stored(first, ends):
        for group in range(2):
            low_part = jnp.zeros((STRIP, LANES), f32)
            high_part = jnp.zeros((STRIP, LANES), f32)
            for index in range(group * per, min(12, (group + 1) * per)):
                slot = index % per
                low_part = jnp.where(lanes // STRIP == slot, ends[index], low_part)
                high_part = jnp.where(lanes // STRIP == (slot - 1) % per, ends[index], high_part)
            span = slice(group * LANES, (group + 1) * LANES)
            near_cols[first : first + STRIP, span] = jnp.where(even_col, high_part, low_part).astype(bf16)
            far_cols[first : first + STRIP, span] = jnp.where(even_col, low_part, high_part).astype(bf16)

    places = list(range(0, rows, STRIP))
    waiting = [rotated(places[0])]
    for index in range(12):
        value = source(index, 0)
        at, _ = row_place(index)
        for piece in range(2):
            firsts[piece, at : at + STRIP, :] = value[:, piece * LANES : (piece + 1) * LANES]
    for index in reversed(range(12)):
        value = source(index, rows - STRIP)
        at, count = row_place(index)
        at = STRIP + at + count - STRIP
        for piece in range(2):
            lasts[piece, at : at + STRIP, :] = value[:, piece * LANES : (piece + 1) * LANES]
    for number, first in enumerate(places):
        if number + 1 < len(places):
            waiting.append(rotated(places[number + 1]))
        stored(first, waiting[number])
    for piece in range(2):
        span = slice(piece * LANES, (piece + 1) * LANES)
        top = firsts[piece, : near_rows.shape[0], :]
        bottom = lasts[piece, STRIP : STRIP + near_rows.shape[0], :]
        near_rows[:, span] = jnp.where(even_row, bottom, top).astype(bf16)
        far_rows[:, span] = jnp.where(even_row, top, bottom).astype(bf16)


class Strips:
    def __init__(self, field, coef):
        self.field, self.coef = field, coef
        self.even_col, self.even_row = is_even("gy"), is_even("gx")
        self.lanes = lane_index(STRIP)

    def place(self, index, first, one, two, ends):
        target = self.field if index < 6 else self.coef
        which = index if index < 6 else index - 6
        factor = FIELD_SCALE[index] if index < 6 else TENSOR_SCALE[index - 6]
        if factor != 1.0:
            one, two, ends = one * factor, two * factor, ends * factor
        count = one.shape[0]
        lane = lane_index(count)
        target[0, which, first : first + count, :] = jnp.where(lane < LANES - STRIP, one, ends)
        target[1, which, first : first + count, :] = jnp.where(lane < LANES // 2, two, one)
        target[2, which, first : first + count, :] = jnp.where(lane < STRIP, ends, two)

    def ends(self, near, far):
        low_strip = jnp.where(self.even_col, far, near)
        high_strip = jnp.where(self.even_col, near, far)
        odd = (self.lanes // STRIP) % 2 == 1
        per = LANES // STRIP
        pairs = []
        for group in range(2):
            low = low_strip[:, group * LANES : (group + 1) * LANES]
            high = high_strip[:, group * LANES : (group + 1) * LANES]
            pairs.append((jnp.where(odd, low, high), jnp.where(odd, high, low)))
        return [shifted(pairs[index // per][index % per % 2], -STRIP * (index % per)) for index in range(12)]


def assemble_kernel(start, tensor, mask, near_cols, far_cols, field, coef, keep, keep2):
    rows, cols = start.shape[1:]
    tiles, deep = field.shape[0], field.shape[2]
    row_base = lax.axis_index("gx") * rows
    col_base = lax.axis_index("gy") * cols
    total_rows = rows * lax.axis_size("gx")
    total_cols = cols * lax.axis_size("gy")
    edge = jnp.zeros((SUB, LANES), f32)
    for tile in range(tiles):
        r = lax.broadcasted_iota(jnp.int32, (deep, LANES), 0) - PAD
        gr, gc = r + row_base, tile_columns(tile, cols, deep) + col_base
        good = (gr >= 0) & (gr < total_rows) & (gc >= 0) & (gc < total_cols)
        keep[tile] = jnp.where(good, 1.0, 0.0)
        keep2[tile] = jnp.where(good, BELOW, 0.0)
        for index in range(6):
            for first in (0, SUB, PAD + rows + SUB, deep - SUB):
                field[tile, index, first : first + SUB, :] = edge
                coef[tile, index, first : first + SUB, :] = edge
    strips = Strips(field, coef)

    def begun(first):
        return strips.ends(
            near_cols[first : first + STRIP, :].astype(f32), far_cols[first : first + STRIP, :].astype(f32)
        )

    def ended(first, ends):
        for index in range(12):
            if index < 6:
                value = start[index, first : first + STRIP, :].astype(f32)
            else:
                value = tensor[index - 6, first : first + STRIP, :].astype(f32)
                if index >= 9:
                    value = value * mask[first : first + STRIP, :]
            strips.place(index, PAD + first, value[:, :LANES], value[:, LANES:], ends[index])

    places = list(range(0, rows, STRIP))
    waiting = [begun(places[0])]
    for number, first in enumerate(places):
        if number + 1 < len(places):
            waiting.append(begun(places[number + 1]))
        ended(first, waiting[number])


def main_kernel(
    field_in, coef_in, keep, keep2, near_rows, far_rows, image, sums, field, coef, flux, inner, wide
):
    rows, cols = image.shape[1:]
    tiles, deep = field.shape[0], field.shape[2]
    bounds = (0, 3 * LANES // 4, cols - 3 * LANES // 4, cols)
    edge = jnp.zeros((SUB, LANES), f32)
    for tile in range(tiles):
        c = tile_columns(tile, cols, SUB)
        inner[tile] = jnp.where((c >= bounds[tile]) & (c < bounds[tile + 1]), 1.0, 0.0)
        for index in range(6):
            for first in (0, SUB, PAD + rows + SUB, deep - SUB):
                flux[tile, index, first : first + SUB, :] = edge
    strips = Strips(field, coef)
    even_row = strips.even_row
    packed = near_rows.shape[0] - 4 * STRIP
    for upper, edge in ((True, PAD), (False, PAD + rows)):
        def rows_of(at, count, upper=upper):
            near, far = near_rows[at : at + count, :].astype(f32), far_rows[at : at + count, :].astype(f32)
            return jnp.where(even_row, far, near) if upper else jnp.where(even_row, near, far)

        corner = packed + (STRIP if upper else 0)
        ends = strips.ends(rows_of(corner, STRIP), rows_of(corner + 2 * STRIP, STRIP))
        level = 0 if upper else 1
        value = rows_of(0, packed)
        for piece in range(2):
            wide[level, piece] = value[:, piece * LANES : (piece + 1) * LANES]
        for index in range(12):
            at, count = row_place(index)
            for begin in (0, count - SUB):
                row = begin + (STRIP - count if upper else 0)
                first = edge + begin - (count if upper else 0)
                span = slice(at + begin, at + begin + SUB)
                strips.place(index, first, wide[level, 0, span, :], wide[level, 1, span, :], ends[index][row : row + SUB])

    def load(ref, tile, index, first, offset):
        return ref[tile, index, pl.ds(first + offset, SUB), :]

    def curl(ref, tile, first, back):
        wanted = (0, 2, 3, 5)
        turn, again = (2, -1) if back else (-2, 1)
        others = {index: shifted(load(ref, tile, index, first, 0), turn) for index in wanted}
        yield None
        near, far = {}, {}
        for index in wanted:
            value, other = load(ref, tile, index, first, 0), others[index]
            near[index] = 27.0 * value + other
            far[index] = shifted(27.0 * other + value, again)
        yield None
        out_parts = []
        for part in range(2):
            xi, yi, zi = 3 * part, 3 * part + 1, 3 * part + 2
            ox, oy = load(ref, tile, 3 - xi, first, 0), load(ref, tile, 4 - xi, first, 0)

            def down(index):
                cells = [load(ref, tile, index, first, step) for step in range(-1 - back, 3 - back)]
                return 27.0 * (cells[2] - cells[1]), cells[3] - cells[0]

            gap, wide = down(zi)
            lean, broad = down(yi)
            hy = (wide - gap) - ox if part == 0 else (wide - gap) + ox
            if back:
                across = near[zi] - far[zi]
                hz = ((lean - broad) - near[xi]) + far[xi]
            else:
                across = far[zi] - near[zi]
                hz = ((lean - broad) + near[xi]) - far[xi]
            hx = across + oy if part == 0 else across - oy
            out_parts.append((hx, hy, hz))
        yield out_parts

    def contract(tile, first, parts):
        k = [load(coef, tile, index, first, 0) for index in range(6)]
        results = []
        for cx, cy, cz in parts:
            results.append(
                (
                    k[0] * cx + k[3] * cy + k[4] * cz,
                    k[3] * cx + k[1] * cy + k[5] * cz,
                    k[4] * cx + k[5] * cy + k[2] * cz,
                )
            )
        return results

    zero = jnp.zeros((SUB, LANES), f32)

    def blocks(low, high):
        return [PAD + low + SUB * number for number in range(-(-(high - low) // SUB))]

    def staged(jobs):
        stages = 3
        for step in range(len(jobs) + (stages - 1) * LAG):
            for stage in range(stages):
                number = step - stage * LAG
                if 0 <= number < len(jobs):
                    next(jobs[number], None)

    def own_rows(first, value):
        low, high = max(0, PAD - first), min(SUB, PAD + rows - first)
        if low == 0 and high == SUB:
            return value
        level = lax.broadcasted_iota(jnp.int32, (SUB, LANES), 0)
        return jnp.where((level >= low) & (level < high), value, 0.0)

    def first_half(tile, first):
        work = curl(field, tile, first, 0)
        next(work)
        yield
        next(work)
        yield
        m, m2 = keep[tile, pl.ds(first, SUB), :], keep2[tile, pl.ds(first, SUB), :]
        for part, (hx, hy, hz) in enumerate(next(work)):
            flux[tile, 3 * part, pl.ds(first, SUB), :] = hx * m2
            flux[tile, 3 * part + 1, pl.ds(first, SUB), :] = hy * m2
            flux[tile, 3 * part + 2, pl.ds(first, SUB), :] = hz * m
        yield

    totals = [zero] * (ITERS + 1)
    running = {}

    def add(number, tile, first, last, flat, upright):
        if first + SUB > PAD and first < PAD + rows:
            flat, upright = own_rows(first, flat), own_rows(first, upright)
            if tile in running:
                flat, upright = running[tile][0] + flat, running[tile][1] + upright
            running[tile] = flat, upright
        if last:
            flat, upright = running.pop(tile)
            if number == ITERS:
                amount = flat + upright * (1.0 / 324.0)
            else:
                amount = flat * (1.0 / 324.0) + upright
            amount = jnp.where(inner[tile] > 0.0, amount, 0.0)
            totals[number] = totals[number] + amount

    def second_half(turn, tile, first, last):
        work = curl(flux, tile, first, 1)
        next(work)
        yield
        next(work)
        yield
        results = contract(tile, first, next(work))
        for part, triple in enumerate(results):
            for axis in range(3):
                field[tile, 3 * part + axis, pl.ds(first, SUB), :] = triple[axis]
        (ax, ay, az), (bx, by, bz) = results
        add(turn, tile, first, last, (ax * ax + ay * ay) + (bx * bx + by * by), az * az + bz * bz)
        yield

    sub_lanes = lane_index(SUB)

    def collect(first):
        yield
        yield
        at = slice(first - PAD, first - PAD + SUB)
        for index in range(6):
            parts = [load(field, tile, index, first, 0) for tile in range(tiles)]
            image[index, at, :LANES] = jnp.where(sub_lanes < bounds[1], parts[0], parts[1])
            image[index, at, LANES:] = jnp.where(sub_lanes < bounds[2] - LANES, parts[1], parts[2])
        yield

    def weigh(tile, first):
        yield
        yield
        e = [load(field, tile, index, first, 0) for index in range(6)]
        parts = contract(tile, first, ((e[0], e[1], BELOW * e[2]), (e[3], e[4], BELOW * e[5])))
        for part, triple in enumerate(parts):
            for axis in range(3):
                flux[tile, 3 * part + axis, pl.ds(first, SUB), :] = triple[axis]
        yield

    def pair(tile, first, last):
        works = curl(field, tile, first, 0), curl(flux, tile, first, 0)
        for _ in range(2):
            for work in works:
                next(work)
            yield
        one, two = next(works[0]), next(works[1])
        flat = (one[0][0] * two[0][0] + one[0][1] * two[0][1]) + (one[1][0] * two[1][0] + one[1][1] * two[1][1])
        upright = one[0][2] * two[0][2] + one[1][2] * two[1][2]
        add(ITERS, tile, first, last, flat, upright)
        yield

    jobs = []
    for turn in range(ITERS):
        reach = 3 * (ITERS - 1 - turn)
        spans = blocks(-3 - reach, rows + 3 + reach), blocks(-1 - reach, rows + 2 + reach)
        jobs += [first_half(tile, first) for tile in range(tiles) for first in spans[0]]
        jobs += [second_half(turn, tile, first, first == spans[1][-1]) for tile in range(tiles) for first in spans[1]]
    jobs += [weigh(tile, first) for tile in range(tiles) for first in blocks(-1, rows + 2)]
    jobs += [collect(first) for first in blocks(0, rows)]
    own = blocks(0, rows)
    jobs += [pair(tile, first, first == own[-1]) for tile in range(tiles) for first in own]
    staged(jobs)

    line_lanes = lax.broadcasted_iota(jnp.int32, (1, LANES), 1)
    line = jnp.zeros((1, LANES), f32)
    for number, total in enumerate(totals):
        amount = jnp.sum(jnp.sum(total, axis=0, keepdims=True), axis=1, keepdims=True)
        line = jnp.where(line_lanes == number, amount, line)
    sums[...] = jnp.broadcast_to(line, sums.shape)


def scale_kernel(cell_count, field, sums, out, estimate):
    totals = jnp.sum(sums[...], axis=0, keepdims=True)
    picks = [totals[:, number : number + 1] for number in range(ITERS + 1)]
    factor = jnp.ones((1, 1), f32)
    for number in range(ITERS):
        square_sum = factor * factor * picks[number]
        factor = factor * lax.rsqrt(square_sum / cell_count + epsilon)
    estimate[...] = picks[ITERS] / picks[ITERS - 1]
    flat = factor * (1.0 / 18.0)
    for index in range(6):
        out[index] = field[index] * (factor if index % 3 == 2 else flat)


def on_device(start_field, tensor, class_map):
    rows, cols = start_field.shape[1:]
    devices = lax.axis_size("gx") * lax.axis_size("gy")
    cell_count = rows * cols * devices
    if cols != 2 * LANES or rows % STRIP:
        raise ValueError("block shape")
    tiles = 3
    whole = pl.BlockSpec(memory_space=pltpu.VMEM)
    strip_rows = -(-6 * (DEEP_FIELD + DEEP_TENSOR) // SUB) * SUB
    anywhere = pl.BlockSpec(memory_space=pltpu.HBM)
    near_cols, far_cols, near_rows, far_rows, *own = pl.pallas_call(
        pack_kernel,
        out_shape=(
            jax.ShapeDtypeStruct((rows, 2 * LANES), bf16),
            jax.ShapeDtypeStruct((rows, 2 * LANES), bf16),
            jax.ShapeDtypeStruct((strip_rows, cols), bf16),
            jax.ShapeDtypeStruct((strip_rows, cols), bf16),
            pltpu.VMEM(start_field.shape, bf16),
            pltpu.VMEM(tensor.shape, bf16),
            pltpu.VMEM((rows, cols), f32),
        ),
        in_specs=[anywhere] * 3,
        out_specs=(whole,) * 7,
        scratch_shapes=[
            pltpu.VMEM(class_map.shape, jnp.int32),
            pltpu.VMEM((2, strip_rows + 2 * STRIP, LANES), f32),
            pltpu.VMEM((2, strip_rows + 2 * STRIP, LANES), f32),
            pltpu.SemaphoreType.DMA((3,)),
        ],
        compiler_params=pltpu.CompilerParams(vmem_limit_bytes=ROOM_SMALL),
        name="pack",
    )(*(pltpu.with_memory_space_constraint(array, pltpu.HBM) for array in (start_field, tensor, class_map)))

    def traded(near, far, axis):
        count = lax.axis_size(axis)
        inward = [(i, i + 1) for i in range(1, count - 1, 2)]
        outward = [(i, i + 1) for i in range(0, count - 1, 2)]
        both = [pairs + [(j, i) for i, j in pairs] for pairs in (outward, inward)]
        far = lax.ppermute(far, axis, both[1])
        return lax.ppermute(near, axis, both[0]), far

    near_cols, far_cols = traded(near_cols, far_cols, "gy")
    corners = [near_cols[:STRIP], near_cols[-STRIP:], far_cols[:STRIP], far_cols[-STRIP:]]
    near_rows = jnp.concatenate([near_rows] + corners)
    far_rows = jnp.concatenate([far_rows] + corners)
    near_rows, far_rows = traded(near_rows, far_rows, "gx")
    deep = rows + 2 * PAD
    stack, plane = (tiles, 6, deep, LANES), (tiles, deep, LANES)
    field, coef, keep, keep2 = pl.pallas_call(
        assemble_kernel,
        out_shape=(pltpu.VMEM(stack, f32), pltpu.VMEM(stack, f32), pltpu.VMEM(plane, f32), pltpu.VMEM(plane, f32)),
        in_specs=[whole] * 5,
        out_specs=(whole,) * 4,
        compiler_params=pltpu.CompilerParams(vmem_limit_bytes=ROOM_SMALL),
        cost_estimate=pl.CostEstimate(flops=2_000_000, bytes_accessed=6_000_000, transcendentals=0),
        name="assemble",
    )(*(pltpu.with_memory_space_constraint(array, pltpu.VMEM) for array in own), near_cols, far_cols)
    held = [pltpu.with_memory_space_constraint(array, pltpu.VMEM) for array in (field, coef)]
    image, sums, _, _ = pl.pallas_call(
        main_kernel,
        out_shape=(
            jax.ShapeDtypeStruct((6, rows, cols), f32),
            jax.ShapeDtypeStruct((devices, LANES), f32),
            pltpu.VMEM(stack, f32),
            pltpu.VMEM(stack, f32),
        ),
        in_specs=[whole] * 6,
        out_specs=(whole,) * 4,
        input_output_aliases={0: 2, 1: 3},
        scratch_shapes=[
            pltpu.VMEM(stack, f32),
            pltpu.VMEM((tiles, SUB, LANES), f32),
            pltpu.VMEM((2, 2, strip_rows, LANES), f32),
        ],
        compiler_params=pltpu.CompilerParams(
            vmem_limit_bytes=ROOM_LARGE
        ),
        name="products",
    )(*held, keep, keep2, near_rows, far_rows)
    sums = lax.all_to_all(sums, ("gx", "gy"), 0, 0, tiled=True)

    def scale(*refs):
        scale_kernel(float(cell_count), *refs)

    mode, estimate = pl.pallas_call(
        scale,
        out_shape=(
            jax.ShapeDtypeStruct((6, rows, cols), f32),
            jax.ShapeDtypeStruct((1, 1), f32),
        ),
        in_specs=[whole] * 2,
        out_specs=(whole,) * 2,
        compiler_params=pltpu.CompilerParams(vmem_limit_bytes=ROOM_SMALL),
        name="scale",
    )(image, sums)
    return mode, estimate[0, 0]


def solution(mesh):
    placed = (P(None, "gx", "gy"), P(None, "gx", "gy"), P("gx", "gy"))
    return jax.shard_map(
        on_device, mesh=mesh, in_specs=placed, out_specs=(P(None, "gx", "gy"), P()), check_vma=False
    )
```

```python
import jax
import jax.numpy as jnp
from jax import lax
from jax.experimental import pallas as pl
from jax.experimental.pallas import tpu as pltpu
from jax.sharding import PartitionSpec as P

TILE = 16
ITERS = 4
LANES = 128
SUB = 8
STRIP = 16
PAD = 24
epsilon = 1e-06
f32 = jnp.float32
bf16 = jnp.bfloat16
FIELD_SCALE = (18.0, 18.0, 1.0, 18.0, 18.0, 1.0)
TENSOR_SCALE = (
    1.0 / 576.0,
    1.0 / 576.0,
    1.0 / (576.0 * 324.0),
    1.0 / 576.0,
    1.0 / (576.0 * 18.0),
    1.0 / (576.0 * 18.0),
)
BELOW = 324.0
DEEP_FIELD = 14
DEEP_TENSOR = 11
LAG = 10
ROOM_SMALL = 8 << 20
ROOM_LARGE = 24 << 20


def row_place(index):
    if index < 6:
        return index * DEEP_FIELD, DEEP_FIELD
    return 6 * DEEP_FIELD + (index - 6) * DEEP_TENSOR, DEEP_TENSOR


def lane_index(rows):
    return lax.broadcasted_iota(jnp.int32, (rows, LANES), 1)


def shifted(value, amount):
    amount = amount % LANES
    return value if amount == 0 else pltpu.roll(value, amount, 1)


def heavy_cells(class_map, rows, cols):
    tiles_x, tiles_y = class_map.shape
    row_of = lax.broadcasted_iota(jnp.int32, (rows, tiles_x), 0) // TILE
    row_pick = (row_of == lax.broadcasted_iota(jnp.int32, (rows, tiles_x), 1)).astype(f32)
    col_of = lax.broadcasted_iota(jnp.int32, (tiles_y, cols), 1) // TILE
    col_pick = (col_of == lax.broadcasted_iota(jnp.int32, (tiles_y, cols), 0)).astype(f32)
    spread = jnp.dot(row_pick, class_map.astype(f32), preferred_element_type=f32)
    return jnp.dot(spread, col_pick, preferred_element_type=f32)


def tile_columns(tile, cols, count):
    c = lane_index(count)
    if tile == 0:
        return jnp.where(c < LANES - STRIP, c, c - LANES)
    if tile == 1:
        return jnp.where(c < LANES // 2, c + LANES, c)
    return jnp.where(c < STRIP, c + cols, c + LANES)


def is_even(axis):
    return lax.rem(lax.axis_index(axis), 2) == 0


def pack_kernel(
    start_in, tensor_in, class_in, near_cols, far_cols, near_rows, far_rows, start, tensor, mask, class_map, firsts, lasts, here
):
    copies = [
        pltpu.make_async_copy(source, target, here.at[number])
        for number, (source, target) in enumerate(((class_in, class_map), (tensor_in, tensor), (start_in, start)))
    ]
    for copy in copies:
        copy.start()
    rows, cols = start.shape[1:]
    even_col, even_row = is_even("gy"), is_even("gx")
    copies[0].wait()
    mask[...] = heavy_cells(class_map[...], rows, cols)
    copies[1].wait()
    copies[2].wait()

    def source(index, first):
        if index < 6:
            return start[index, first : first + STRIP, :].astype(f32)
        value = tensor[index - 6, first : first + STRIP, :].astype(f32)
        if index >= 9:
            value = value * mask[first : first + STRIP, :]
        return value

    lanes = lane_index(STRIP)
    per = LANES // STRIP

    def rotated(first):
        ends = []
        for index in range(12):
            value = source(index, first)
            value = jnp.where(lanes < LANES // 2, value[:, :LANES], value[:, LANES:])
            ends.append(shifted(value, STRIP * (index % per)))
        return ends

    def stored(first, ends):
        for group in range(2):
            low_part = jnp.zeros((STRIP, LANES), f32)
            high_part = jnp.zeros((STRIP, LANES), f32)
            for index in range(group * per, min(12, (group + 1) * per)):
                slot = index % per
                low_part = jnp.where(lanes // STRIP == slot, ends[index], low_part)
                high_part = jnp.where(lanes // STRIP == (slot - 1) % per, ends[index], high_part)
            span = slice(group * LANES, (group + 1) * LANES)
            near_cols[first : first + STRIP, span] = jnp.where(even_col, high_part, low_part).astype(bf16)
            far_cols[first : first + STRIP, span] = jnp.where(even_col, low_part, high_part).astype(bf16)

    places = list(range(0, rows, STRIP))
    waiting = [rotated(places[0])]
    for index in range(12):
        value = source(index, 0)
        at, _ = row_place(index)
        for piece in range(2):
            firsts[piece, at : at + STRIP, :] = value[:, piece * LANES : (piece + 1) * LANES]
    for index in reversed(range(12)):
        value = source(index, rows - STRIP)
        at, count = row_place(index)
        at = STRIP + at + count - STRIP
        for piece in range(2):
            lasts[piece, at : at + STRIP, :] = value[:, piece * LANES : (piece + 1) * LANES]
    for number, first in enumerate(places):
        if number + 1 < len(places):
            waiting.append(rotated(places[number + 1]))
        stored(first, waiting[number])
    for piece in range(2):
        span = slice(piece * LANES, (piece + 1) * LANES)
        top = firsts[piece, : near_rows.shape[0], :]
        bottom = lasts[piece, STRIP : STRIP + near_rows.shape[0], :]
        near_rows[:, span] = jnp.where(even_row, bottom, top).astype(bf16)
        far_rows[:, span] = jnp.where(even_row, top, bottom).astype(bf16)


class Strips:
    def __init__(self, field, coef):
        self.field, self.coef = field, coef
        self.even_col, self.even_row = is_even("gy"), is_even("gx")
        self.lanes = lane_index(STRIP)

    def place(self, index, first, one, two, ends):
        target = self.field if index < 6 else self.coef
        which = index if index < 6 else index - 6
        factor = FIELD_SCALE[index] if index < 6 else TENSOR_SCALE[index - 6]
        if factor != 1.0:
            one, two, ends = one * factor, two * factor, ends * factor
        count = one.shape[0]
        lane = lane_index(count)
        target[0, which, first : first + count, :] = jnp.where(lane < LANES - STRIP, one, ends)
        target[1, which, first : first + count, :] = jnp.where(lane < LANES // 2, two, one)
        target[2, which, first : first + count, :] = jnp.where(lane < STRIP, ends, two)

    def ends(self, near, far):
        low_strip = jnp.where(self.even_col, far, near)
        high_strip = jnp.where(self.even_col, near, far)
        odd = (self.lanes // STRIP) % 2 == 1
        per = LANES // STRIP
        pairs = []
        for group in range(2):
            low = low_strip[:, group * LANES : (group + 1) * LANES]
            high = high_strip[:, group * LANES : (group + 1) * LANES]
            pairs.append((jnp.where(odd, low, high), jnp.where(odd, high, low)))
        return [shifted(pairs[index // per][index % per % 2], -STRIP * (index % per)) for index in range(12)]


def load(ref, tile, index, first, offset):
    return ref[tile, index, pl.ds(first + offset, SUB), :]


def curl(ref, tile, first, back):
    wanted = (0, 2, 3, 5)
    turn, again = (2, -1) if back else (-2, 1)
    others = {index: shifted(load(ref, tile, index, first, 0), turn) for index in wanted}
    yield None
    near, far = {}, {}
    for index in wanted:
        value, other = load(ref, tile, index, first, 0), others[index]
        near[index] = 27.0 * value + other
        far[index] = shifted(27.0 * other + value, again)
    yield None
    out_parts = []
    for part in range(2):
        xi, yi, zi = 3 * part, 3 * part + 1, 3 * part + 2
        ox, oy = load(ref, tile, 3 - xi, first, 0), load(ref, tile, 4 - xi, first, 0)

        def down(index):
            cells = [load(ref, tile, index, first, step) for step in range(-1 - back, 3 - back)]
            return 27.0 * (cells[2] - cells[1]), cells[3] - cells[0]

        gap, wide = down(zi)
        lean, broad = down(yi)
        hy = (wide - gap) - ox if part == 0 else (wide - gap) + ox
        if back:
            across = near[zi] - far[zi]
            hz = ((lean - broad) - near[xi]) + far[xi]
        else:
            across = far[zi] - near[zi]
            hz = ((lean - broad) + near[xi]) - far[xi]
        hx = across + oy if part == 0 else across - oy
        out_parts.append((hx, hy, hz))
    yield out_parts


def blocks(low, high):
    return [PAD + low + SUB * number for number in range(-(-(high - low) // SUB))]


def staged(jobs):
    stages = 3
    for step in range(len(jobs) + (stages - 1) * LAG):
        for stage in range(stages):
            number = step - stage * LAG
            if 0 <= number < len(jobs):
                next(jobs[number], None)


def first_half(field, flux, keep, keep2, tile, first):
    work = curl(field, tile, first, 0)
    next(work)
    yield
    next(work)
    yield
    m, m2 = keep[tile, pl.ds(first, SUB), :], keep2[tile, pl.ds(first, SUB), :]
    for part, (hx, hy, hz) in enumerate(next(work)):
        flux[tile, 3 * part, pl.ds(first, SUB), :] = hx * m2
        flux[tile, 3 * part + 1, pl.ds(first, SUB), :] = hy * m2
        flux[tile, 3 * part + 2, pl.ds(first, SUB), :] = hz * m
    yield


def first_spans(rows):
    reach = 3 * (ITERS - 1)
    one, two = blocks(-3 - reach, rows + 3 + reach), blocks(-1 - reach, rows + 2 + reach)
    inside = [first for first in one if first - 1 >= PAD and first + SUB + 2 <= PAD + rows]
    ready = [first for first in two if first - 2 >= inside[0] and first + SUB + 1 <= inside[-1] + SUB]
    return one, two, inside, ready


def assemble_kernel(start, tensor, mask, near_cols, far_cols, field, coef, keep, keep2, flux):
    rows, cols = start.shape[1:]
    tiles, deep = field.shape[0], field.shape[2]
    row_base = lax.axis_index("gx") * rows
    col_base = lax.axis_index("gy") * cols
    total_rows = rows * lax.axis_size("gx")
    total_cols = cols * lax.axis_size("gy")
    edge = jnp.zeros((SUB, LANES), f32)
    for tile in range(tiles):
        r = lax.broadcasted_iota(jnp.int32, (deep, LANES), 0) - PAD
        gr, gc = r + row_base, tile_columns(tile, cols, deep) + col_base
        good = (gr >= 0) & (gr < total_rows) & (gc >= 0) & (gc < total_cols)
        keep[tile] = jnp.where(good, 1.0, 0.0)
        keep2[tile] = jnp.where(good, BELOW, 0.0)
        for index in range(6):
            for first in (0, SUB, PAD + rows + SUB, deep - SUB):
                field[tile, index, first : first + SUB, :] = edge
                coef[tile, index, first : first + SUB, :] = edge
    strips = Strips(field, coef)

    def begun(first):
        return strips.ends(
            near_cols[first : first + STRIP, :].astype(f32), far_cols[first : first + STRIP, :].astype(f32)
        )

    def ended(first, ends):
        for index in range(12):
            if index < 6:
                value = start[index, first : first + STRIP, :].astype(f32)
            else:
                value = tensor[index - 6, first : first + STRIP, :].astype(f32)
                if index >= 9:
                    value = value * mask[first : first + STRIP, :]
            strips.place(index, PAD + first, value[:, :LANES], value[:, LANES:], ends[index])

    places = list(range(0, rows, STRIP))
    waiting = [begun(places[0])]
    for number, first in enumerate(places):
        if number + 1 < len(places):
            waiting.append(begun(places[number + 1]))
        ended(first, waiting[number])
    inside = first_spans(rows)[2]
    staged([first_half(field, flux, keep, keep2, tile, first) for tile in range(tiles) for first in inside])


def main_kernel(
    field_in, coef_in, flux_in, keep, keep2, near_rows, far_rows, image, sums, field, coef, flux, inner, wide
):
    rows, cols = image.shape[1:]
    tiles, deep = field.shape[0], field.shape[2]
    bounds = (0, 3 * LANES // 4, cols - 3 * LANES // 4, cols)
    edge = jnp.zeros((SUB, LANES), f32)
    for tile in range(tiles):
        c = tile_columns(tile, cols, SUB)
        inner[tile] = jnp.where((c >= bounds[tile]) & (c < bounds[tile + 1]), 1.0, 0.0)
        for index in range(6):
            for first in (0, SUB, PAD + rows + SUB, deep - SUB):
                flux[tile, index, first : first + SUB, :] = edge
    strips = Strips(field, coef)
    even_row = strips.even_row
    packed = near_rows.shape[0] - 4 * STRIP
    for upper, edge in ((True, PAD), (False, PAD + rows)):
        def rows_of(at, count, upper=upper):
            near, far = near_rows[at : at + count, :].astype(f32), far_rows[at : at + count, :].astype(f32)
            return jnp.where(even_row, far, near) if upper else jnp.where(even_row, near, far)

        corner = packed + (STRIP if upper else 0)
        ends = strips.ends(rows_of(corner, STRIP), rows_of(corner + 2 * STRIP, STRIP))
        level = 0 if upper else 1
        value = rows_of(0, packed)
        for piece in range(2):
            wide[level, piece] = value[:, piece * LANES : (piece + 1) * LANES]
        for index in range(12):
            at, count = row_place(index)
            for begin in (0, count - SUB):
                row = begin + (STRIP - count if upper else 0)
                first = edge + begin - (count if upper else 0)
                span = slice(at + begin, at + begin + SUB)
                strips.place(index, first, wide[level, 0, span, :], wide[level, 1, span, :], ends[index][row : row + SUB])

    def contract(tile, first, parts):
        k = [load(coef, tile, index, first, 0) for index in range(6)]
        results = []
        for cx, cy, cz in parts:
            results.append(
                (
                    k[0] * cx + k[3] * cy + k[4] * cz,
                    k[3] * cx + k[1] * cy + k[5] * cz,
                    k[4] * cx + k[5] * cy + k[2] * cz,
                )
            )
        return results

    zero = jnp.zeros((SUB, LANES), f32)

    def own_rows(first, value):
        low, high = max(0, PAD - first), min(SUB, PAD + rows - first)
        if low == 0 and high == SUB:
            return value
        level = lax.broadcasted_iota(jnp.int32, (SUB, LANES), 0)
        return jnp.where((level >= low) & (level < high), value, 0.0)

    totals = [zero] * (ITERS + 1)
    running = {}

    def add(number, tile, first, last, flat, upright):
        if first + SUB > PAD and first < PAD + rows:
            flat, upright = own_rows(first, flat), own_rows(first, upright)
            if tile in running:
                flat, upright = running[tile][0] + flat, running[tile][1] + upright
            running[tile] = flat, upright
        if last:
            flat, upright = running.pop(tile)
            if number == ITERS:
                amount = flat + upright * (1.0 / 324.0)
            else:
                amount = flat * (1.0 / 324.0) + upright
            amount = jnp.where(inner[tile] > 0.0, amount, 0.0)
            totals[number] = totals[number] + amount

    def second_half(turn, tile, first, last):
        work = curl(flux, tile, first, 1)
        next(work)
        yield
        next(work)
        yield
        results = contract(tile, first, next(work))
        for part, triple in enumerate(results):
            for axis in range(3):
                field[tile, 3 * part + axis, pl.ds(first, SUB), :] = triple[axis]
        (ax, ay, az), (bx, by, bz) = results
        add(turn, tile, first, last, (ax * ax + ay * ay) + (bx * bx + by * by), az * az + bz * bz)
        yield

    sub_lanes = lane_index(SUB)

    def collect(first):
        yield
        yield
        at = slice(first - PAD, first - PAD + SUB)
        for index in range(6):
            parts = [load(field, tile, index, first, 0) for tile in range(tiles)]
            image[index, at, :LANES] = jnp.where(sub_lanes < bounds[1], parts[0], parts[1])
            image[index, at, LANES:] = jnp.where(sub_lanes < bounds[2] - LANES, parts[1], parts[2])
        yield

    def weigh(tile, first):
        yield
        yield
        e = [load(field, tile, index, first, 0) for index in range(6)]
        parts = contract(tile, first, ((e[0], e[1], BELOW * e[2]), (e[3], e[4], BELOW * e[5])))
        for part, triple in enumerate(parts):
            for axis in range(3):
                flux[tile, 3 * part + axis, pl.ds(first, SUB), :] = triple[axis]
        yield

    def pair(tile, first, last):
        works = curl(field, tile, first, 0), curl(flux, tile, first, 0)
        for _ in range(2):
            for work in works:
                next(work)
            yield
        one, two = next(works[0]), next(works[1])
        flat = (one[0][0] * two[0][0] + one[0][1] * two[0][1]) + (one[1][0] * two[1][0] + one[1][1] * two[1][1])
        upright = one[0][2] * two[0][2] + one[1][2] * two[1][2]
        add(ITERS, tile, first, last, flat, upright)
        yield

    jobs = []
    for turn in range(ITERS):
        reach = 3 * (ITERS - 1 - turn)
        spans = blocks(-3 - reach, rows + 3 + reach), blocks(-1 - reach, rows + 2 + reach)
        ones = [(tile, first) for tile in range(tiles) for first in spans[0]]
        twos = [(tile, first) for tile in range(tiles) for first in spans[1]]
        if turn == 0:
            inside, ready = first_spans(rows)[2:]
            ones = [(tile, first) for tile, first in ones if first not in inside]
            edges = [(tile, first) for tile, first in twos if first not in ready]
            calm = [(tile, first) for tile, first in twos if first in ready]
            twos = calm[: len(calm) // 2] + edges + calm[len(calm) // 2 :]
        jobs += [first_half(field, flux, keep, keep2, *spot) for spot in ones]
        final = {tile: number for number, (tile, _) in enumerate(twos)}
        jobs += [second_half(turn, *spot, number == final[spot[0]]) for number, spot in enumerate(twos)]
    jobs += [weigh(tile, first) for tile in range(tiles) for first in blocks(-1, rows + 2)]
    jobs += [collect(first) for first in blocks(0, rows)]
    own = blocks(0, rows)
    jobs += [pair(tile, first, first == own[-1]) for tile in range(tiles) for first in own]
    staged(jobs)

    line_lanes = lax.broadcasted_iota(jnp.int32, (1, LANES), 1)
    line = jnp.zeros((1, LANES), f32)
    for number, total in enumerate(totals):
        amount = jnp.sum(jnp.sum(total, axis=0, keepdims=True), axis=1, keepdims=True)
        line = jnp.where(line_lanes == number, amount, line)
    sums[...] = jnp.broadcast_to(line, sums.shape)


def scale_kernel(cell_count, field, sums, out, estimate):
    totals = jnp.sum(sums[...], axis=0, keepdims=True)
    picks = [totals[:, number : number + 1] for number in range(ITERS + 1)]
    factor = jnp.ones((1, 1), f32)
    for number in range(ITERS):
        square_sum = factor * factor * picks[number]
        factor = factor * lax.rsqrt(square_sum / cell_count + epsilon)
    estimate[...] = picks[ITERS] / picks[ITERS - 1]
    flat = factor * (1.0 / 18.0)
    for index in range(6):
        out[index] = field[index] * (factor if index % 3 == 2 else flat)


def on_device(start_field, tensor, class_map):
    rows, cols = start_field.shape[1:]
    devices = lax.axis_size("gx") * lax.axis_size("gy")
    cell_count = rows * cols * devices
    if cols != 2 * LANES or rows % STRIP:
        raise ValueError("block shape")
    tiles = 3
    whole = pl.BlockSpec(memory_space=pltpu.VMEM)
    strip_rows = -(-6 * (DEEP_FIELD + DEEP_TENSOR) // SUB) * SUB
    anywhere = pl.BlockSpec(memory_space=pltpu.HBM)
    near_cols, far_cols, near_rows, far_rows, *own = pl.pallas_call(
        pack_kernel,
        out_shape=(
            jax.ShapeDtypeStruct((rows, 2 * LANES), bf16),
            jax.ShapeDtypeStruct((rows, 2 * LANES), bf16),
            jax.ShapeDtypeStruct((strip_rows, cols), bf16),
            jax.ShapeDtypeStruct((strip_rows, cols), bf16),
            pltpu.VMEM(start_field.shape, bf16),
            pltpu.VMEM(tensor.shape, bf16),
            pltpu.VMEM((rows, cols), f32),
        ),
        in_specs=[anywhere] * 3,
        out_specs=(whole,) * 7,
        scratch_shapes=[
            pltpu.VMEM(class_map.shape, jnp.int32),
            pltpu.VMEM((2, strip_rows + 2 * STRIP, LANES), f32),
            pltpu.VMEM((2, strip_rows + 2 * STRIP, LANES), f32),
            pltpu.SemaphoreType.DMA((3,)),
        ],
        compiler_params=pltpu.CompilerParams(vmem_limit_bytes=ROOM_SMALL),
        name="pack",
    )(*(pltpu.with_memory_space_constraint(array, pltpu.HBM) for array in (start_field, tensor, class_map)))

    def traded(near, far, axis):
        count = lax.axis_size(axis)
        inward = [(i, i + 1) for i in range(1, count - 1, 2)]
        outward = [(i, i + 1) for i in range(0, count - 1, 2)]
        both = [pairs + [(j, i) for i, j in pairs] for pairs in (outward, inward)]
        far = lax.ppermute(far, axis, both[1])
        return lax.ppermute(near, axis, both[0]), far

    near_cols, far_cols = traded(near_cols, far_cols, "gy")
    corners = [near_cols[:STRIP], near_cols[-STRIP:], far_cols[:STRIP], far_cols[-STRIP:]]
    near_rows = jnp.concatenate([near_rows] + corners)
    far_rows = jnp.concatenate([far_rows] + corners)
    near_rows, far_rows = traded(near_rows, far_rows, "gx")
    deep = rows + 2 * PAD
    stack, plane = (tiles, 6, deep, LANES), (tiles, deep, LANES)
    field, coef, keep, keep2, flux = pl.pallas_call(
        assemble_kernel,
        out_shape=tuple(pltpu.VMEM(shape, f32) for shape in (stack, stack, plane, plane, stack)),
        in_specs=[whole] * 5,
        out_specs=(whole,) * 5,
        compiler_params=pltpu.CompilerParams(
            vmem_limit_bytes=ROOM_SMALL
        ),
        cost_estimate=pl.CostEstimate(flops=2_000_000, bytes_accessed=6_000_000, transcendentals=0),
        name="assemble",
    )(*(pltpu.with_memory_space_constraint(array, pltpu.VMEM) for array in own), near_cols, far_cols)
    held = [pltpu.with_memory_space_constraint(array, pltpu.VMEM) for array in (field, coef, flux)]
    image, sums, *_ = pl.pallas_call(
        main_kernel,
        out_shape=(
            jax.ShapeDtypeStruct((6, rows, cols), f32),
            jax.ShapeDtypeStruct((devices, LANES), f32),
            pltpu.VMEM(stack, f32),
            pltpu.VMEM(stack, f32),
            pltpu.VMEM(stack, f32),
        ),
        in_specs=[whole] * 7,
        out_specs=(whole,) * 5,
        input_output_aliases={0: 2, 1: 3, 2: 4},
        scratch_shapes=[
            pltpu.VMEM((tiles, SUB, LANES), f32),
            pltpu.VMEM((2, 2, strip_rows, LANES), f32),
        ],
        compiler_params=pltpu.CompilerParams(
            vmem_limit_bytes=ROOM_LARGE
        ),
        name="products",
    )(*held, keep, keep2, near_rows, far_rows)
    sums = lax.all_to_all(sums, ("gx", "gy"), 0, 0, tiled=True)

    def scale(*refs):
        scale_kernel(float(cell_count), *refs)

    mode, estimate = pl.pallas_call(
        scale,
        out_shape=(
            jax.ShapeDtypeStruct((6, rows, cols), f32),
            jax.ShapeDtypeStruct((1, 1), f32),
        ),
        in_specs=[whole] * 2,
        out_specs=(whole,) * 2,
        compiler_params=pltpu.CompilerParams(vmem_limit_bytes=ROOM_SMALL),
        name="scale",
    )(image, sums)
    return mode, estimate[0, 0]


def solution(mesh):
    placed = (P(None, "gx", "gy"), P(None, "gx", "gy"), P("gx", "gy"))
    return jax.shard_map(
        on_device, mesh=mesh, in_specs=placed, out_specs=(P(None, "gx", "gy"), P()), check_vma=False
    )
```
